32 devices in a mesh: cp: 16 (over z, y, core), vocab: 2 (over x).
Axes of the slice: x: 2, y: 2, z: 4, core: 2. Of those that a mesh axis runs over, the one named last changes fastest.
Arguments:
- queries: bfloat16 [2048, 4096], P('cp', 'vocab'), may hold values from -160 to 160
- key_states: bfloat16 [2048, 1024], P('cp', 'vocab'), may hold values from -6 to 6
- value_states: bfloat16 [2048, 1024], P('cp', 'vocab'), may hold values from -6 to 6
- out_grad: bfloat16 [2048, 4096], P('cp', 'vocab'), may hold values from -6 to 6
- o_weight: bfloat16 [4096, 4096], P('vocab'), may hold values from -0.09375 to 0.09375
- span_order: int32 [32], replicated, may hold values from 0 to 31, each once
Outputs:
- query_grad: float32 [2048, 4096], P('cp', 'vocab')
- key_grad: float32 [2048, 1024], P('cp', 'vocab')
- value_grad: float32 [2048, 1024], P('cp', 'vocab')
The draws below stay inside these ranges and needn't reach their ends.
Inputs may be any that keep to these rules, and one draw needn't show every extreme that they name: `span_order`: each of the 32 span indices once.
All inputs are finite; a program needn't handle non-finite values.
Results may differ from the reference program's by a relative error of at most 0.014.
Values may be sent and summed in bfloat16 or wider, within the bound.
A program may use at most 64 MiB of HBM per device.

```python
import jax
import jax.numpy as jnp
from jax import lax

D = 4096
HEADS = 32
KV_HEADS = 8
HEAD_DIM = 128
TOK_DEV = 128
SEQ = 2048
SPANS = 32


def attention_pair(key):
    base_key = jax.random.fold_in(key, 7101)
    split_keys = jax.random.split(base_key, 2)
    key_values = jnp.clip(jax.random.normal(split_keys[0], (SEQ, KV_HEADS, 1, HEAD_DIM), jnp.float32), -6.0, 6.0)
    query_values = jnp.clip(jax.random.normal(split_keys[1], (SEQ, KV_HEADS, HEADS // KV_HEADS, HEAD_DIM), jnp.float32), -6.0, 6.0)
    return (query_values.reshape(SEQ, HEADS * HEAD_DIM), key_values.reshape(SEQ, KV_HEADS * HEAD_DIM))


def draw_queries(key, part):
    return attention_pair(key)[0].astype(jnp.bfloat16)


def draw_key_states(key, part):
    return attention_pair(key)[1].astype(jnp.bfloat16)


def level_of(own_key, dims, shards, low, largest):
    def one(axis_at, parts):
        steps = jax.random.uniform(jax.random.fold_in(jax.random.fold_in(own_key, 6), axis_at), (parts,), jnp.float32, low / len(shards), largest / len(shards))
        return jnp.repeat(jnp.exp(steps), dims[axis_at] // parts).reshape((-1,) + (1,) * (len(dims) - axis_at - 1))

    gain = one(*shards[0])
    for cut in shards[1:]:
        gain = gain * one(*cut)
    return gain


def bell_draw(rng, dims, scale, limit, pieces=(), held_as=jnp.bfloat16):
    drawn = jax.random.normal(rng, dims, jnp.float32) * scale
    if len(pieces) > 0:
        drawn = level_of(rng, dims, pieces, -0.22, 0.18) * drawn
    return jnp.clip(drawn, min=-limit, max=limit).astype(held_as)


def setup_inputs(seed: int = 0) -> dict:
    key_of = jax.random.split(jax.random.key(seed), 7)
    return {
        "queries": draw_queries(jax.random.fold_in(key_of[6], 71), 0),
        "key_states": draw_key_states(jax.random.fold_in(key_of[6], 71), 0),
        "value_states": bell_draw(key_of[2], (SEQ, KV_HEADS * HEAD_DIM), 1.0, 6.0, ((0, 16), (1, 2))),
        "out_grad": bell_draw(key_of[3], (SEQ, D), 1.0, 6.0, ((0, 16), (1, 2))),
        "o_weight": bell_draw(key_of[4], (HEADS * HEAD_DIM, D), D ** -0.5, 0.09375, ((0, 2),)),
        "span_order": jax.random.permutation(key_of[5], SPANS).astype(jnp.int32),
    }


def positions(span_order, span_rows):
    offsets = jnp.arange(span_rows, dtype=jnp.int32)
    return (span_order.astype(jnp.int32)[:, None] * span_rows + offsets[None, :]).reshape(-1)


def attention_grads(queries, key_states, value_states, upstream, places):
    seq_len = queries.shape[0]
    groups = HEADS // KV_HEADS
    factor = HEAD_DIM ** -0.5
    block_rows = TOK_DEV * 8
    block_count = seq_len // block_rows
    query_heads = queries.reshape(seq_len, KV_HEADS, groups, HEAD_DIM).transpose(1, 2, 0, 3).astype(jnp.float32)
    upstream_heads = upstream.reshape(seq_len, KV_HEADS, groups, HEAD_DIM).transpose(1, 2, 0, 3).astype(jnp.float32)
    key_heads = key_states.reshape(seq_len, KV_HEADS, HEAD_DIM).transpose(1, 0, 2).astype(jnp.float32)
    value_heads = value_states.reshape(seq_len, KV_HEADS, HEAD_DIM).transpose(1, 0, 2).astype(jnp.float32)

    def one_head(operands):
        head_queries, head_upstream, head_keys, head_values = operands

        def block_step(carried, block_index):
            key_total, value_total = carried
            offset = block_index * block_rows
            rows_query = lax.dynamic_slice_in_dim(head_queries, offset, block_rows, 1)
            rows_upstream = lax.dynamic_slice_in_dim(head_upstream, offset, block_rows, 1)
            query_places = lax.dynamic_slice_in_dim(places, offset, block_rows, 0)
            visible = places[None, :] <= query_places[:, None]
            scores = jnp.einsum("gqd,sd->gqs", rows_query, head_keys) * factor
            scores = jnp.where(visible[None], scores, -jnp.inf)
            row_peak = jnp.max(scores, axis=2, keepdims=True)
            logsum = row_peak + jnp.log(jnp.sum(jnp.exp(scores - row_peak), axis=2, keepdims=True))
            weights = jnp.exp(scores - logsum)
            grad_probs = jnp.einsum("gqd,sd->gqs", rows_upstream, head_values)
            deltas = jnp.sum(weights * grad_probs, axis=2, keepdims=True)
            grad_scores = lax.optimization_barrier((weights * (grad_probs - deltas)).astype(jnp.bfloat16)).astype(jnp.float32)
            weights_low = lax.optimization_barrier(weights.astype(jnp.bfloat16)).astype(jnp.float32)
            query_block = jnp.einsum("gqs,sd->gqd", grad_scores, head_keys) * factor
            key_total = key_total + jnp.einsum("gqs,gqd->sd", grad_scores, rows_query) * factor
            value_total = value_total + jnp.einsum("gqs,gqd->sd", weights_low, rows_upstream)
            return (key_total, value_total), query_block

        zeros = jnp.zeros((seq_len, HEAD_DIM), jnp.float32)
        (key_total, value_total), query_stack = lax.scan(block_step, (zeros, zeros), jnp.arange(block_count, dtype=jnp.int32))
        query_total = query_stack.transpose(1, 0, 2, 3).reshape(groups, seq_len, HEAD_DIM)
        return key_total, value_total, query_total

    key_grads, value_grads, query_grads = lax.map(one_head, (query_heads, upstream_heads, key_heads, value_heads))
    query_grad = query_grads.transpose(2, 0, 1, 3).reshape(seq_len, HEADS * HEAD_DIM)
    key_grad = key_grads.transpose(1, 0, 2).reshape(seq_len, KV_HEADS * HEAD_DIM)
    value_grad = value_grads.transpose(1, 0, 2).reshape(seq_len, KV_HEADS * HEAD_DIM)
    return query_grad, key_grad, value_grad


def reference(queries, key_states, value_states, out_grad, o_weight, span_order):
    upstream = lax.dot_general(out_grad, o_weight, (((1,), (1,)), ((), ())), preferred_element_type=jnp.float32).astype(jnp.bfloat16)
    places = positions(span_order, TOK_DEV // 2)
    query_grad, key_grad, value_grad = attention_grads(queries, key_states, value_states, upstream, places)
    return query_grad, key_grad, value_grad
```

```python
import functools

import jax
import jax.numpy as jnp
from jax import lax
from jax.experimental import pallas as pl
from jax.experimental.pallas import tpu as pltpu
from jax.sharding import PartitionSpec as P

HEADS = 32
KV_HEADS = 8
HEAD_DIM = 128


def positions(span_order, span_rows):
    offsets = jnp.arange(span_rows, dtype=jnp.int32)
    return (span_order[:, None] * span_rows + offsets[None, :]).reshape(-1)


def block_scores(query_block, key_block, query_places, key_places, factor):
    scores = (
        jnp.einsum("qkgd,skd->kgqs", query_block, key_block, preferred_element_type=jnp.float32)
        * factor
    )
    visible = key_places[None, :] <= query_places[:, None]
    return jnp.where(visible, scores, -jnp.inf)


def local(queries, key_states, value_states, out_grad, o_weight, span_order):
    own_rows = queries.shape[0]
    kv_width = key_states.shape[1]
    kv_heads = kv_width // HEAD_DIM
    groups = HEADS // KV_HEADS
    factor = HEAD_DIM ** (-0.5)
    upstream = lax.dot_general(
        lax.all_gather(out_grad, "vocab", axis=1, tiled=True),
        o_weight,
        (((1,), (1,)), ((), ())),
        preferred_element_type=jnp.float32,
    ).astype(jnp.bfloat16)
    places = positions(span_order, own_rows // 2)
    seq_len = places.shape[0]
    own_places = lax.dynamic_slice_in_dim(places, lax.axis_index("cp") * own_rows, own_rows, 0)
    query_heads = queries.reshape(own_rows, kv_heads, groups, HEAD_DIM)
    upstream_heads = upstream.reshape(own_rows, kv_heads, groups, HEAD_DIM)
    key_all, value_all = (
        lax.all_gather(key_states, "cp", axis=0, tiled=True),
        lax.all_gather(value_states, "cp", axis=0, tiled=True),
    )
    key_all = key_all.reshape(seq_len, kv_heads, HEAD_DIM)
    value_all = value_all.reshape(seq_len, kv_heads, HEAD_DIM)
    block_rows = own_rows * 8
    block_count = seq_len // block_rows
    block_ids = jnp.arange(block_count, dtype=jnp.int32)
    stat_shape = (kv_heads, groups, own_rows)

    def key_block(block_index):
        offset = block_index * block_rows
        return (
            lax.dynamic_slice_in_dim(key_all, offset, block_rows, 0),
            lax.dynamic_slice_in_dim(value_all, offset, block_rows, 0),
            lax.dynamic_slice_in_dim(places, offset, block_rows, 0),
        )

    def stats_step(carried, block_index):
        running, totals, delta_acc = carried
        keys_now, values_now, places_now = key_block(block_index)
        scores = block_scores(query_heads, keys_now, own_places, places_now, factor)
        newest = jnp.maximum(running, jnp.max(scores, axis=3))
        rescale = jnp.exp(running - newest)
        raised = jnp.exp(scores - newest[..., None])
        grad_probs = jnp.einsum(
            "qkgd,skd->kgqs", upstream_heads, values_now, preferred_element_type=jnp.float32
        )
        totals = totals * rescale + jnp.sum(raised, axis=3)
        delta_acc = delta_acc * rescale + jnp.sum(raised * grad_probs, axis=3)
        return ((newest, totals, delta_acc), None)

    start_stats = (
        jnp.full(stat_shape, -1e30, jnp.float32),
        jnp.zeros(stat_shape, jnp.float32),
        jnp.zeros(stat_shape, jnp.float32),
    )
    (running, totals, delta_acc), unused = lax.scan(stats_step, start_stats, block_ids)
    logsum = running + jnp.log(totals)
    deltas = delta_acc / totals

    def grad_pieces(block_index):
        keys_now, values_now, places_now = key_block(block_index)
        scores = block_scores(query_heads, keys_now, own_places, places_now, factor)
        weights = jnp.exp(scores - logsum[..., None])
        grad_probs = jnp.einsum(
            "qkgd,skd->kgqs", upstream_heads, values_now, preferred_element_type=jnp.float32
        )
        grad_scores = (weights * (grad_probs - deltas[..., None])).astype(jnp.bfloat16)
        return (keys_now, weights, grad_scores)

    query_zeros = jnp.zeros((own_rows, kv_heads, groups, HEAD_DIM), jnp.float32)

    def grad_step(carried, block_index):
        keys_now, weights, grad_scores = grad_pieces(block_index)
        carried = (
            carried
            + jnp.einsum(
                "kgqs,skd->qkgd", grad_scores, keys_now, preferred_element_type=jnp.float32
            )
            * factor
        )
        key_term = (
            jnp.einsum(
                "kgqs,qkgd->skd", grad_scores, query_heads, preferred_element_type=jnp.float32
            )
            * factor
        )
        value_term = jnp.einsum(
            "kgqs,qkgd->skd",
            weights.astype(jnp.bfloat16),
            upstream_heads,
            preferred_element_type=jnp.float32,
        )
        joined = jnp.concatenate(
            (key_term.reshape(block_rows, kv_width), value_term.reshape(block_rows, kv_width)),
            axis=1,
        )
        return (carried, joined)

    query_total, stacked = lax.scan(grad_step, query_zeros, block_ids)
    terms = stacked.reshape(seq_len, 2 * kv_width)
    mine = lax.psum_scatter(
        terms.astype(jnp.bfloat16), "cp", scatter_dimension=0, tiled=True
    ).astype(jnp.float32)
    key_grad = mine[:, :kv_width]
    value_grad = mine[:, kv_width:]
    query_grad = query_total.reshape(own_rows, kv_heads * groups * HEAD_DIM)
    return (query_grad, key_grad, value_grad)


MESH = pl.DeviceIdType.MESH
NT = (((1,), (1,)), ((), ()))
NN = (((1,), (0,)), ((), ()))
TILE = 256


def dot(a, b, dims):
    return lax.dot_general(a, b, dims, preferred_element_type=jnp.float32)


def neighbours(mine):
    partner = mine + 1 - 2 * lax.rem(mine, 2)
    return [mine, partner, lax.rem(mine + 2, 4), lax.rem(partner + 2, 4)]


def signal(peer):
    pl.semaphore_signal(
        pltpu.get_barrier_semaphore(), inc=1, device_id=peer, device_id_type=MESH
    )


def columns(ref, at, size):
    return ref.at[:, pl.ds(pl.multiple_of(at * size, size), size)]


def send_kernel(
    planes, kv_heads, cuts, q_ref, k_ref, v_ref, g_ref, w_ref, q_all, k_all, v_all, u_all,
    own_q, own_k, own_v, own_g, other_g, own_w, other_w, partial, u_buf,
    load_sem, own_sem, w_sem, g_sem, plane_sem, line_sem, kv_sem, q_sems, u_sems,
):
    me = lax.axis_index("cp")
    half = lax.axis_index("vocab")
    mine = lax.rem(me, kv_heads)
    plane = me // kv_heads
    first = plane * kv_heads
    end = planes - 1
    width = g_ref.shape[1]
    wide = width // kv_heads
    cut = wide // 2
    peers = neighbours(mine)
    order = [2, 3, 1, 0]
    steps = [(idx, part) for idx in order for part in range(2)]

    def w_copy(t, own):
        idx, part = steps[t]
        side = half if own else 1 - half
        return pltpu.make_async_copy(
            w_ref.at[
                pl.ds(pl.multiple_of(peers[idx] * wide + part * cut, cut), cut),
                pl.ds(pl.multiple_of(side * width, width), width),
            ],
            (own_w if own else other_w).at[t],
            w_sem.at[0 if own else 1, t],
        )

    loads = [
        pltpu.make_async_copy(source, target, load_sem.at[i])
        for i, (source, target) in enumerate(
            ((g_ref, own_g), (k_ref, own_k), (v_ref, own_v), (q_ref, own_q))
        )
    ]
    for copy in loads:
        copy.start()
    own_copies = [
        pltpu.make_async_copy(columns(q_ref, mine, wide), q_all.at[mine], own_sem.at[0]),
        pltpu.make_async_copy(columns(k_ref, mine, HEAD_DIM), k_all.at[me], own_sem.at[1]),
        pltpu.make_async_copy(columns(v_ref, mine, HEAD_DIM), v_all.at[me], own_sem.at[2]),
    ]
    for copy in own_copies:
        copy.start()
    for own in (True, False):
        for t in range(len(steps)):
            w_copy(t, own).start()

    signal({"vocab": 1 - half})
    for peer in peers[1:]:
        signal({"cp": first + peer})

    @pl.when(plane < end)
    def _():
        signal({"cp": me + kv_heads})

    @pl.when(plane > 0)
    def _():
        signal({"cp": me - kv_heads})

    lines = jnp.minimum(plane, 1) + jnp.minimum(end - plane, 1)
    pl.semaphore_wait(pltpu.get_barrier_semaphore(), kv_heads + lines)
    for copy in loads:
        copy.wait()

    def g_copy(r):
        rows = pl.ds(*cuts[r])
        return pltpu.make_async_remote_copy(
            src_ref=own_g.at[rows], dst_ref=other_g.at[rows],
            send_sem=g_sem.at[0, r], recv_sem=g_sem.at[1, r],
            device_id={"vocab": 1 - half}, device_id_type=MESH,
        )

    def plane_copy(idx, i):
        return pltpu.make_async_remote_copy(
            src_ref=columns((own_k, own_v)[i], peers[idx], HEAD_DIM),
            dst_ref=(k_all, v_all)[i].at[me],
            send_sem=plane_sem.at[i, idx], recv_sem=kv_sem.at[i, me],
            device_id={"cp": first + peers[idx]}, device_id_type=MESH,
        )

    def line_copy(left, hops, idx, i):
        block = me - mine + peers[idx] + (kv_heads if left else -kv_heads) * hops
        kept = (k_all, v_all)[i]
        own = hops == 0 and idx == 0
        return pltpu.make_async_remote_copy(
            src_ref=columns((own_k, own_v)[i], mine, HEAD_DIM) if own else kept.at[block],
            dst_ref=kept.at[block],
            send_sem=line_sem.at[left, i, hops * kv_heads + idx], recv_sem=kv_sem.at[i, block],
            device_id={"cp": me + (-kv_heads if left else kv_heads)}, device_id_type=MESH,
        )

    def arrived(block):
        for i in range(2):
            slot = (k_all, v_all)[i].at[block]
            pltpu.make_async_remote_copy(
                src_ref=slot, dst_ref=slot,
                send_sem=plane_sem.at[i, 0], recv_sem=kv_sem.at[i, block],
                device_id={"cp": first + peers[1]}, device_id_type=MESH,
            ).wait_recv()

    def start_line(left, hops, idx):
        for i in range(2):
            line_copy(left, hops, idx, i).start()

    def open_line(idx):
        @pl.when(plane < end)
        def _():
            start_line(0, 0, idx)

        @pl.when(plane > 0)
        def _():
            start_line(1, 0, idx)

    def pass_plane(idx):
        arrived(first + peers[idx])
        open_line(idx)

    def pass_line(hops, idx):
        @pl.when((plane >= hops) & (plane < end))
        def _():
            arrived(first + peers[idx] - hops * kv_heads)
            start_line(0, hops, idx)

        @pl.when((plane <= end - hops) & (plane > 0))
        def _():
            arrived(first + peers[idx] + hops * kv_heads)
            start_line(1, hops, idx)

    def q_copy(idx):
        return pltpu.make_async_remote_copy(
            src_ref=columns(own_q, peers[idx], wide), dst_ref=q_all.at[mine],
            send_sem=q_sems.at[0, idx], recv_sem=q_sems.at[1, idx],
            device_id={"cp": first + peers[idx]}, device_id_type=MESH,
        )

    def u_copy(r, idx):
        rows = pl.ds(*cuts[r])
        return pltpu.make_async_remote_copy(
            src_ref=u_buf.at[idx, rows], dst_ref=u_all.at[mine, rows],
            send_sem=u_sems.at[0, r, idx], recv_sem=u_sems.at[1, r, idx],
            device_id={"cp": first + peers[idx]}, device_id_type=MESH,
        )

    for r in range(len(cuts)):
        g_copy(r).start()
    open_line(0)
    for idx in order[:-1]:
        for i in range(2):
            plane_copy(idx, i).start()
    for idx in order[:-1]:
        q_copy(idx).start()

    half_way = len(steps) // 2
    for t in range(len(steps)):
        w_copy(t, True).wait()
        partial[t] = dot(own_g[...], own_w[t], NT)
        if t == half_way - 1:
            pass_plane(1)
    pass_plane(2)
    pass_plane(3)
    events = [(hops, idx) for hops in range(1, end) for idx in range(kv_heads)]
    slots = len(cuts) * len(steps) // 2
    done = 0
    for r, (start, size) in enumerate(cuts):
        rows = pl.ds(start, size)
        g_copy(r).wait_recv()
        for t, (idx, part) in enumerate(steps):
            if r == 0:
                w_copy(t, False).wait()
            block = partial[t, rows] + dot(other_g[rows], other_w[t], NT)
            u_buf[idx, rows, pl.ds(part * cut, cut)] = block.astype(jnp.bfloat16)
            if part == 1:
                if idx != 0:
                    u_copy(r, idx).start()
                at = r * len(steps) // 2 + t // 2 + 1
                while done < len(events) and done * slots < at * len(events):
                    pass_line(*events[done])
                    done += 1
    for hops, idx in events[done:]:
        pass_line(hops, idx)
    u_all[mine] = u_buf[0]

    for hops in range(1, planes):
        for idx in range(kv_heads):
            @pl.when(plane == end)
            def _():
                arrived(first + peers[idx] - hops * kv_heads)

            @pl.when(plane == 0)
            def _():
                arrived(first + peers[idx] + hops * kv_heads)

    for idx in order[:-1]:
        q_copy(idx).wait_recv()
        for r in range(len(cuts)):
            u_copy(r, idx).wait()
    for copy in own_copies:
        copy.wait()
    for r in range(len(cuts)):
        g_copy(r).wait_send()
    for idx in order[:-1]:
        q_copy(idx).wait_send()
        for i in range(2):
            plane_copy(idx, i).wait_send()
    for hops in range(end):
        for idx in range(kv_heads):
            for i in range(2):
                @pl.when((plane >= hops) & (plane < end))
                def _():
                    line_copy(0, hops, idx, i).wait_send()

                @pl.when((plane <= end - hops) & (plane > 0))
                def _():
                    line_copy(1, hops, idx, i).wait_send()


def score_kernel(
    order_ref, q_ref, k_ref, v_ref, u_ref, w_out, g_out, q_stack, u_stack,
    places, ks, vs, s_buf, p_buf,
):
    plane = lax.axis_index("cp") // q_ref.shape[0]
    own_rows = q_ref.shape[1]
    groups = q_ref.shape[2] // HEAD_DIM
    seq = k_ref.shape[0]
    spans = order_ref.shape[0]
    rows = seq // spans
    tile = groups * rows
    own_spans = q_ref.shape[0] * own_rows // rows
    per_block = own_rows // rows
    per_tile = TILE // rows
    scale = HEAD_DIM ** (-0.5) * 1.4426950408889634

    for r in range(spans):
        places[order_ref[r]] = r

    def place(j):
        return pl.ds(pl.multiple_of(places[j] * rows, rows), rows)

    for j in range(spans):
        for target, ref in ((ks, k_ref), (vs, v_ref)):
            target[pl.ds(j * rows, rows), :] = ref[place(j), :]

    def fold(x, op):
        return op(x.reshape(TILE // 8, 8, tile), axis=0)

    key_at = lax.broadcasted_iota(jnp.int32, (TILE, tile), 0)
    query_at = lax.rem(lax.broadcasted_iota(jnp.int32, (TILE, tile), 1), rows)

    def one_span(t, carry):
        block = t // per_block
        own = pl.ds(pl.multiple_of(lax.rem(t, per_block) * rows, rows), rows)
        cols = pl.ds(pl.multiple_of(t * tile, tile), tile)
        start = order_ref[plane * own_spans + t] * rows

        def stacked(ref):
            return jnp.concatenate(
                [ref[block, own, h * HEAD_DIM : (h + 1) * HEAD_DIM] for h in range(groups)], axis=0
            )

        def with_keys(last):
            q_tile = stacked(q_ref)
            u_tile = stacked(u_ref)
            q_stack[cols, :] = q_tile
            u_stack[cols, :] = u_tile
            peak = None
            for j in range(last + 1):
                keys = pl.ds(j * TILE, TILE)
                s = dot(ks[keys, :], q_tile, NT)
                if j == last:
                    s = jnp.where(key_at + (last * TILE - start) <= query_at, s, -1e30)
                s_buf[keys, :] = s
                top = fold(s, jnp.max)
                peak = top if peak is None else jnp.maximum(peak, top)
            peak = jnp.max(peak, axis=0, keepdims=True)
            total = jnp.zeros((8, tile), jnp.float32)
            delta = jnp.zeros((8, tile), jnp.float32)
            for j in range(last + 1):
                keys = pl.ds(j * TILE, TILE)
                p = jnp.exp2((s_buf[keys, :] - peak) * scale)
                dp = dot(vs[keys, :], u_tile, NT)
                total = total + fold(p, jnp.sum)
                delta = delta + fold(p * dp, jnp.sum)
                s_buf[keys, :] = p
                p_buf[keys, :] = dp
            inverse = 1.0 / jnp.sum(total, axis=0, keepdims=True)
            delta = jnp.sum(delta, axis=0, keepdims=True) * inverse
            for j in range(last + 1):
                keys = pl.ds(j * TILE, TILE)
                w = s_buf[keys, :] * inverse
                g = (w * (p_buf[keys, :] - delta)).astype(jnp.bfloat16)
                w = w.astype(jnp.bfloat16)
                for i in range(per_tile):
                    at = place(j * per_tile + i)
                    w_out[at, cols] = w[i * rows : (i + 1) * rows]
                    g_out[at, cols] = g[i * rows : (i + 1) * rows]
            blank = jnp.zeros((rows, tile), jnp.bfloat16)
            for j in range((last + 1) * per_tile, spans):
                w_out[place(j), cols] = blank
                g_out[place(j), cols] = blank

        for last in range(seq // TILE):
            pl.when(start // TILE == last)(functools.partial(with_keys, last))
        return carry

    lax.fori_loop(0, own_spans, one_span, 0)


def return_kernel(
    planes, kv_heads, w_ref, g_ref, q_ref, u_ref, k_ref, dq_all, dk_out, dv_out,
    k_turned, terms, summed, inbox, plane_box, dq_buf,
    send_sem, recv_sem, plane_sems, q_sems,
):
    me = lax.axis_index("cp")
    mine = lax.rem(me, kv_heads)
    plane = me // kv_heads
    first = plane * kv_heads
    end = planes - 1
    high = plane // 2
    outer = (plane == 0) | (plane == end)
    inner = 2 - high
    near = 1 + high
    peers = neighbours(mine)
    block_rows, wide = dq_buf.shape[1:]
    groups = wide // HEAD_DIM
    seq = g_ref.shape[0]
    tile = 2 * HEAD_DIM
    rows = tile // groups
    factor = HEAD_DIM ** (-0.5)

    for peer in peers[1:]:
        signal({"cp": first + peer})

    @pl.when(plane < end)
    def _():
        for m in range(kv_heads):
            signal({"cp": first + kv_heads + m})

    @pl.when(plane > 0)
    def _():
        for m in range(kv_heads):
            signal({"cp": first - kv_heads + m})

    def remote(source, target, sent, got, device):
        return pltpu.make_async_remote_copy(
            src_ref=source, dst_ref=target, send_sem=sent, recv_sem=got,
            device_id={"cp": device}, device_id_type=MESH,
        )

    def relay(source, stage, j, way, hops, device):
        slot = hops * kv_heads + j
        return remote(
            source, inbox.at[way, slot], send_sem.at[stage, j], recv_sem.at[way, slot],
            device * kv_heads + mine,
        )

    def final(source, stage, j, way, device):
        return remote(
            source, inbox.at[way, mine], send_sem.at[stage, j], recv_sem.at[way, mine],
            device * kv_heads + j,
        )

    def arrived(way, slot):
        at = inbox.at[way, slot]
        remote(at, at, send_sem.at[0, 0], recv_sem.at[way, slot], first + peers[1]).wait_recv()

    def chunk_of(i):
        return (1 - high) * (end - i) + high * i

    def compute(i):
        def one(j, carry):
            block = chunk_of(i) * kv_heads + j
            keys = pl.ds(pl.multiple_of(block * block_rows, block_rows), block_rows)
            dk = dot(g_ref[keys, :], q_ref[...], NN) * factor
            dv = dot(w_ref[keys, :], u_ref[...], NN)
            terms[block, :, :HEAD_DIM] = dk.astype(jnp.bfloat16)
            terms[block, :, HEAD_DIM:] = dv.astype(jnp.bfloat16)
            return carry

        lax.fori_loop(0, kv_heads, one, 0)

    def outward(i, j):
        source = terms.at[chunk_of(i) * kv_heads + j]
        if i == end - 1:
            return final(source, i, j, high, near)
        return relay(source, i, j, high, end - 1 - i, near)

    def plane_copy(idx):
        return remote(
            terms.at[first + peers[idx]], plane_box.at[mine],
            plane_sems.at[0, idx], plane_sems.at[1, mine], first + peers[idx],
        )

    def plane_arrived(idx):
        at = plane_box.at[peers[idx]]
        remote(at, at, plane_sems.at[0, idx], plane_sems.at[1, peers[idx]], first + peers[idx]).wait_recv()

    def dq_copy(idx):
        return remote(
            dq_buf.at[peers[idx]], columns(dq_all, mine, wide),
            q_sems.at[0, idx], q_sems.at[1, idx], first + peers[idx],
        )

    for i in range(planes):
        compute(i)
        if i == 0:
            lines = jnp.minimum(plane, 1) + jnp.minimum(end - plane, 1)
            pl.semaphore_wait(
                pltpu.get_barrier_semaphore(), kv_heads - 1 + kv_heads * lines
            )
        if i < end:
            @pl.when(outer)
            def _():
                for j in range(kv_heads):
                    outward(i, j).start()
    for idx in (2, 3, 1):
        plane_copy(idx).start()

    def middle(stage, way, slot, chunk, copy):
        for j in range(kv_heads):
            arrived(way, slot * kv_heads + j)
            total = terms[chunk * kv_heads + j].astype(jnp.float32) + inbox[
                way, slot * kv_heads + j
            ].astype(jnp.float32)
            summed[stage, j] = total.astype(jnp.bfloat16)
            copy(j).start()

    def onward(j):
        return relay(summed.at[0, j], 0, j, high, 1, inner)

    def to_end(j):
        return final(summed.at[1, j], 1, j, 1 - high, high * end)

    def to_inner(j):
        return final(summed.at[2, j], 2, j, high, inner)

    k_turned[...] = k_ref[...].T
    for t in range(seq // tile):
        cols = slice(t * tile, (t + 1) * tile)
        part = dot(k_turned[...], g_ref[:, cols], NN)
        part = (part.T * factor).astype(jnp.bfloat16)
        block, at = divmod(t * rows, block_rows)
        for h in range(groups):
            dq_buf[block, at : at + rows, h * HEAD_DIM : (h + 1) * HEAD_DIM] = part[
                h * rows : (h + 1) * rows
            ]
    for idx in (2, 3, 1):
        dq_copy(idx).start()

    @pl.when(jnp.logical_not(outer))
    def _():
        middle(0, high, 2, (1 - high) * end, onward)
        middle(1, 1 - high, 1, high * end, to_end)
        middle(2, high, 1, inner, to_inner)

    dq_all[:, pl.ds(pl.multiple_of(mine * wide, wide), wide)] = dq_buf[mine]
    plane_box[mine] = terms[me]

    def add(ref, m, value, fresh):
        cols = slice(m * HEAD_DIM, (m + 1) * HEAD_DIM)
        ref[:, cols] = value if fresh else ref[:, cols] + value

    def collect(box, m, fresh):
        value = box.astype(jnp.float32)
        add(dk_out, m, value[:, :HEAD_DIM], fresh)
        add(dv_out, m, value[:, HEAD_DIM:], fresh)

    for idx in range(1, kv_heads):
        plane_arrived(idx)
    for m in range(kv_heads):
        collect(plane_box[m], m, True)

    @pl.when(plane < end)
    def _():
        for m in range(kv_heads):
            arrived(1, m)
            collect(inbox[1, m], m, False)

    @pl.when(plane > 0)
    def _():
        for m in range(kv_heads):
            arrived(0, m)
            collect(inbox[0, m], m, False)

    for idx in range(1, kv_heads):
        plane_copy(idx).wait_send()
        dq_copy(idx).wait()

    @pl.when(outer)
    def _():
        for i in range(end):
            for j in range(kv_heads):
                outward(i, j).wait_send()

    @pl.when(jnp.logical_not(outer))
    def _():
        for copy in (onward, to_end, to_inner):
            for j in range(kv_heads):
                copy(j).wait_send()


def by_planes(n, queries, key_states, value_states, out_grad, o_weight, span_order):
    own_rows, width = queries.shape
    kv_heads = key_states.shape[1] // HEAD_DIM
    planes = n // kv_heads
    wide = width // kv_heads
    cut = wide // 2
    seq = own_rows * n
    tile = (HEADS // KV_HEADS) * (seq // span_order.shape[0])
    stack = kv_heads * own_rows * (HEADS // KV_HEADS)
    quarter = own_rows // 4
    cuts = ((0, 2 * quarter), (2 * quarter, quarter), (3 * quarter, quarter))
    any_spec = pl.BlockSpec(memory_space=pl.ANY)
    vmem_spec = pl.BlockSpec(memory_space=pltpu.VMEM)
    smem_spec = pl.BlockSpec(memory_space=pltpu.SMEM)
    dma = pltpu.SemaphoreType.DMA
    low = jnp.bfloat16
    q_block = pltpu.VMEM((kv_heads, own_rows, wide), low)
    kv_block = pltpu.VMEM((n, own_rows, HEAD_DIM), low)
    q_all, k_all, v_all, u_all = pl.pallas_call(
        functools.partial(send_kernel, planes, kv_heads, cuts),
        out_shape=(q_block, kv_block, kv_block, q_block),
        in_specs=[any_spec] * 5,
        out_specs=(vmem_spec,) * 4,
        scratch_shapes=[
            pltpu.VMEM((own_rows, width), low),
            pltpu.VMEM(key_states.shape, low),
            pltpu.VMEM(key_states.shape, low),
            pltpu.VMEM((own_rows, width), low),
            pltpu.VMEM((own_rows, width), low),
            pltpu.VMEM((2 * kv_heads, cut, width), low),
            pltpu.VMEM((2 * kv_heads, cut, width), low),
            pltpu.VMEM((2 * kv_heads, own_rows, cut), jnp.float32),
            pltpu.VMEM((kv_heads, own_rows, wide), low),
            dma((4,)),
            dma((3,)),
            dma((2, 2 * kv_heads)),
            dma((2, len(cuts))),
            dma((2, kv_heads)),
            dma((2, 2, (planes - 1) * kv_heads)),
            dma((2, n)),
            dma((2, kv_heads)),
            dma((2, len(cuts), kv_heads)),
        ],
        compiler_params=pltpu.CompilerParams(
            collective_id=0, has_side_effects=True, vmem_limit_bytes=SEND_LIMIT
        ),
        name="send_heads",
    )(queries, key_states, value_states, out_grad, o_weight)
    k_all = k_all.reshape(seq, HEAD_DIM)
    pair = jax.ShapeDtypeStruct((seq, stack), low)
    side = jax.ShapeDtypeStruct((stack, HEAD_DIM), low)
    weights, grads, q_stack, u_stack = pl.pallas_call(
        score_kernel,
        out_shape=(pair, pair, side, side),
        in_specs=[smem_spec] + [vmem_spec] * 4,
        out_specs=(vmem_spec,) * 4,
        scratch_shapes=[pltpu.SMEM(span_order.shape, jnp.int32)]
        + [pltpu.VMEM((seq, HEAD_DIM), low)] * 2
        + [pltpu.VMEM((seq, tile), jnp.float32)] * 2,
        compiler_params=pltpu.CompilerParams(vmem_limit_bytes=16 << 20),
        name="scores",
    )(span_order, q_all, k_all, v_all.reshape(seq, HEAD_DIM), u_all)
    term = (own_rows, 2 * HEAD_DIM)
    grad = jax.ShapeDtypeStruct(key_states.shape, jnp.float32)
    dq_all, key_grad, value_grad = pl.pallas_call(
        functools.partial(return_kernel, planes, kv_heads),
        out_shape=(jax.ShapeDtypeStruct((own_rows, width), low), grad, grad),
        in_specs=[vmem_spec] * 5,
        out_specs=(vmem_spec,) * 3,
        scratch_shapes=[
            pltpu.VMEM((HEAD_DIM, seq), low),
            pltpu.VMEM((n,) + term, low),
            pltpu.VMEM((3, kv_heads) + term, low),
            pltpu.VMEM((2, 3 * kv_heads) + term, low),
            pltpu.VMEM((kv_heads,) + term, low),
            pltpu.VMEM((kv_heads, own_rows, wide), low),
            dma((3, kv_heads)),
            dma((2, 3 * kv_heads)),
            dma((2, kv_heads)),
            dma((2, kv_heads)),
        ],
        compiler_params=pltpu.CompilerParams(
            collective_id=1, has_side_effects=True, vmem_limit_bytes=16 << 20
        ),
        name="return_grads",
    )(weights, grads, q_stack, u_stack, k_all)
    return (dq_all.astype(jnp.float32), key_grad, value_grad)


SEND_LIMIT = 60 << 20


def solution(mesh):
    n = mesh.shape["cp"]
    planes = mesh.shape["vocab"] == 2 and n == 4 * (KV_HEADS // 2)
    body = functools.partial(by_planes, n) if planes else local
    return jax.shard_map(
        body,
        mesh=mesh,
        in_specs=(
            P("cp", "vocab"),
            P("cp", "vocab"),
            P("cp", "vocab"),
            P("cp", "vocab"),
            P("vocab", None),
            P(),
        ),
        out_specs=(P("cp", "vocab"), P("cp", "vocab"), P("cp", "vocab")),
        check_vma=False,
    )
```

```python
import functools

import jax
import jax.numpy as jnp
from jax import lax
from jax.experimental import pallas as pl
from jax.experimental.pallas import tpu as pltpu
from jax.sharding import PartitionSpec as P

HEADS = 32
KV_HEADS = 8
HEAD_DIM = 128


def positions(span_order, span_rows):
    offsets = jnp.arange(span_rows, dtype=jnp.int32)
    return (span_order[:, None] * span_rows + offsets[None, :]).reshape(-1)


def block_scores(query_block, key_block, query_places, key_places, factor):
    scores = (
        jnp.einsum("qkgd,skd->kgqs", query_block, key_block, preferred_element_type=jnp.float32)
        * factor
    )
    visible = key_places[None, :] <= query_places[:, None]
    return jnp.where(visible, scores, -jnp.inf)


def local(queries, key_states, value_states, out_grad, o_weight, span_order):
    own_rows = queries.shape[0]
    kv_width = key_states.shape[1]
    kv_heads = kv_width // HEAD_DIM
    groups = HEADS // KV_HEADS
    factor = HEAD_DIM ** (-0.5)
    upstream = lax.dot_general(
        lax.all_gather(out_grad, "vocab", axis=1, tiled=True),
        o_weight,
        (((1,), (1,)), ((), ())),
        preferred_element_type=jnp.float32,
    ).astype(jnp.bfloat16)
    places = positions(span_order, own_rows // 2)
    seq_len = places.shape[0]
    own_places = lax.dynamic_slice_in_dim(places, lax.axis_index("cp") * own_rows, own_rows, 0)
    query_heads = queries.reshape(own_rows, kv_heads, groups, HEAD_DIM)
    upstream_heads = upstream.reshape(own_rows, kv_heads, groups, HEAD_DIM)
    key_all, value_all = (
        lax.all_gather(key_states, "cp", axis=0, tiled=True),
        lax.all_gather(value_states, "cp", axis=0, tiled=True),
    )
    key_all = key_all.reshape(seq_len, kv_heads, HEAD_DIM)
    value_all = value_all.reshape(seq_len, kv_heads, HEAD_DIM)
    block_rows = own_rows * 8
    block_count = seq_len // block_rows
    block_ids = jnp.arange(block_count, dtype=jnp.int32)
    stat_shape = (kv_heads, groups, own_rows)

    def key_block(block_index):
        offset = block_index * block_rows
        return (
            lax.dynamic_slice_in_dim(key_all, offset, block_rows, 0),
            lax.dynamic_slice_in_dim(value_all, offset, block_rows, 0),
            lax.dynamic_slice_in_dim(places, offset, block_rows, 0),
        )

    def stats_step(carried, block_index):
        running, totals, delta_acc = carried
        keys_now, values_now, places_now = key_block(block_index)
        scores = block_scores(query_heads, keys_now, own_places, places_now, factor)
        newest = jnp.maximum(running, jnp.max(scores, axis=3))
        rescale = jnp.exp(running - newest)
        raised = jnp.exp(scores - newest[..., None])
        grad_probs = jnp.einsum(
            "qkgd,skd->kgqs", upstream_heads, values_now, preferred_element_type=jnp.float32
        )
        totals = totals * rescale + jnp.sum(raised, axis=3)
        delta_acc = delta_acc * rescale + jnp.sum(raised * grad_probs, axis=3)
        return ((newest, totals, delta_acc), None)

    start_stats = (
        jnp.full(stat_shape, -1e30, jnp.float32),
        jnp.zeros(stat_shape, jnp.float32),
        jnp.zeros(stat_shape, jnp.float32),
    )
    (running, totals, delta_acc), unused = lax.scan(stats_step, start_stats, block_ids)
    logsum = running + jnp.log(totals)
    deltas = delta_acc / totals

    def grad_pieces(block_index):
        keys_now, values_now, places_now = key_block(block_index)
        scores = block_scores(query_heads, keys_now, own_places, places_now, factor)
        weights = jnp.exp(scores - logsum[..., None])
        grad_probs = jnp.einsum(
            "qkgd,skd->kgqs", upstream_heads, values_now, preferred_element_type=jnp.float32
        )
        grad_scores = (weights * (grad_probs - deltas[..., None])).astype(jnp.bfloat16)
        return (keys_now, weights, grad_scores)

    query_zeros = jnp.zeros((own_rows, kv_heads, groups, HEAD_DIM), jnp.float32)

    def grad_step(carried, block_index):
        keys_now, weights, grad_scores = grad_pieces(block_index)
        carried = (
            carried
            + jnp.einsum(
                "kgqs,skd->qkgd", grad_scores, keys_now, preferred_element_type=jnp.float32
            )
            * factor
        )
        key_term = (
            jnp.einsum(
                "kgqs,qkgd->skd", grad_scores, query_heads, preferred_element_type=jnp.float32
            )
            * factor
        )
        value_term = jnp.einsum(
            "kgqs,qkgd->skd",
            weights.astype(jnp.bfloat16),
            upstream_heads,
            preferred_element_type=jnp.float32,
        )
        joined = jnp.concatenate(
            (key_term.reshape(block_rows, kv_width), value_term.reshape(block_rows, kv_width)),
            axis=1,
        )
        return (carried, joined)

    query_total, stacked = lax.scan(grad_step, query_zeros, block_ids)
    terms = stacked.reshape(seq_len, 2 * kv_width)
    mine = lax.psum_scatter(
        terms.astype(jnp.bfloat16), "cp", scatter_dimension=0, tiled=True
    ).astype(jnp.float32)
    key_grad = mine[:, :kv_width]
    value_grad = mine[:, kv_width:]
    query_grad = query_total.reshape(own_rows, kv_heads * groups * HEAD_DIM)
    return (query_grad, key_grad, value_grad)


MESH = pl.DeviceIdType.MESH
NT = (((1,), (1,)), ((), ()))
NN = (((1,), (0,)), ((), ()))
TILE = 256


def dot(a, b, dims):
    return lax.dot_general(a, b, dims, preferred_element_type=jnp.float32)


def neighbours(mine):
    partner = mine + 1 - 2 * lax.rem(mine, 2)
    return [mine, partner, lax.rem(mine + 2, 4), lax.rem(partner + 2, 4)]


def signal(peer):
    pl.semaphore_signal(
        pltpu.get_barrier_semaphore(), inc=1, device_id=peer, device_id_type=MESH
    )


def columns(ref, at, size):
    return ref.at[:, pl.ds(pl.multiple_of(at * size, size), size)]


def send_kernel(
    planes, kv_heads, cuts, q_ref, k_ref, v_ref, g_ref, w_ref, q_all, k_all, v_all, u_all,
    own_q, own_k, own_v, own_g, other_g, own_w, other_w, partial, u_buf,
    load_sem, own_sem, w_sem, g_sem, plane_sem, line_sem, kv_sem, q_sems, u_sems,
):
    me = lax.axis_index("cp")
    half = lax.axis_index("vocab")
    mine = lax.rem(me, kv_heads)
    plane = me // kv_heads
    first = plane * kv_heads
    end = planes - 1
    width = g_ref.shape[1]
    wide = width // kv_heads
    cut = wide // 2
    peers = neighbours(mine)
    order = [2, 3, 1, 0]
    steps = [(idx, part) for idx in order for part in range(2)]

    def w_copy(t, own):
        idx, part = steps[t]
        side = half if own else 1 - half
        return pltpu.make_async_copy(
            w_ref.at[
                pl.ds(pl.multiple_of(peers[idx] * wide + part * cut, cut), cut),
                pl.ds(pl.multiple_of(side * width, width), width),
            ],
            (own_w if own else other_w).at[t],
            w_sem.at[0 if own else 1, t],
        )

    loads = [
        pltpu.make_async_copy(source, target, load_sem.at[i])
        for i, (source, target) in enumerate(
            ((g_ref, own_g), (k_ref, own_k), (v_ref, own_v), (q_ref, own_q))
        )
    ]
    for copy in loads:
        copy.start()
    own_copies = [
        pltpu.make_async_copy(columns(q_ref, mine, wide), q_all.at[mine], own_sem.at[0]),
        pltpu.make_async_copy(columns(k_ref, mine, HEAD_DIM), k_all.at[me], own_sem.at[1]),
        pltpu.make_async_copy(columns(v_ref, mine, HEAD_DIM), v_all.at[me], own_sem.at[2]),
    ]
    for copy in own_copies:
        copy.start()
    signal({"vocab": 1 - half})
    for peer in peers[1:]:
        signal({"cp": first + peer})

    @pl.when(plane < end)
    def _():
        signal({"cp": me + kv_heads})

    @pl.when(plane > 0)
    def _():
        signal({"cp": me - kv_heads})

    lines = jnp.minimum(plane, 1) + jnp.minimum(end - plane, 1)
    for copy in loads:
        copy.wait()
    for own in (True, False):
        for t in range(len(steps)):
            w_copy(t, own).start()
    pl.semaphore_wait(pltpu.get_barrier_semaphore(), kv_heads + lines)

    def g_copy(r):
        rows = pl.ds(*cuts[r])
        return pltpu.make_async_remote_copy(
            src_ref=own_g.at[rows], dst_ref=other_g.at[rows],
            send_sem=g_sem.at[0, r], recv_sem=g_sem.at[1, r],
            device_id={"vocab": 1 - half}, device_id_type=MESH,
        )

    def plane_copy(idx, i):
        return pltpu.make_async_remote_copy(
            src_ref=columns((own_k, own_v)[i], peers[idx], HEAD_DIM),
            dst_ref=(k_all, v_all)[i].at[me],
            send_sem=plane_sem.at[i, idx], recv_sem=kv_sem.at[i, me],
            device_id={"cp": first + peers[idx]}, device_id_type=MESH,
        )

    def line_copy(left, hops, idx, i):
        block = me - mine + peers[idx] + (kv_heads if left else -kv_heads) * hops
        kept = (k_all, v_all)[i]
        own = hops == 0 and idx == 0
        return pltpu.make_async_remote_copy(
            src_ref=columns((own_k, own_v)[i], mine, HEAD_DIM) if own else kept.at[block],
            dst_ref=kept.at[block],
            send_sem=line_sem.at[left, i, hops * kv_heads + idx], recv_sem=kv_sem.at[i, block],
            device_id={"cp": me + (-kv_heads if left else kv_heads)}, device_id_type=MESH,
        )

    def arrived(block):
        for i in range(2):
            slot = (k_all, v_all)[i].at[block]
            pltpu.make_async_remote_copy(
                src_ref=slot, dst_ref=slot,
                send_sem=plane_sem.at[i, 0], recv_sem=kv_sem.at[i, block],
                device_id={"cp": first + peers[1]}, device_id_type=MESH,
            ).wait_recv()

    def start_line(left, hops, idx):
        for i in range(2):
            line_copy(left, hops, idx, i).start()

    def open_line(idx):
        @pl.when(plane < end)
        def _():
            start_line(0, 0, idx)

        @pl.when(plane > 0)
        def _():
            start_line(1, 0, idx)

    def pass_plane(idx):
        arrived(first + peers[idx])
        open_line(idx)

    def pass_line(hops, idx):
        @pl.when((plane >= hops) & (plane < end))
        def _():
            arrived(first + peers[idx] - hops * kv_heads)
            start_line(0, hops, idx)

        @pl.when((plane <= end - hops) & (plane > 0))
        def _():
            arrived(first + peers[idx] + hops * kv_heads)
            start_line(1, hops, idx)

    def q_copy(idx):
        return pltpu.make_async_remote_copy(
            src_ref=columns(own_q, peers[idx], wide), dst_ref=q_all.at[mine],
            send_sem=q_sems.at[0, idx], recv_sem=q_sems.at[1, idx],
            device_id={"cp": first + peers[idx]}, device_id_type=MESH,
        )

    def u_copy(r, idx):
        rows = pl.ds(*cuts[r])
        return pltpu.make_async_remote_copy(
            src_ref=u_buf.at[idx, rows], dst_ref=u_all.at[mine, rows],
            send_sem=u_sems.at[0, r, idx], recv_sem=u_sems.at[1, r, idx],
            device_id={"cp": first + peers[idx]}, device_id_type=MESH,
        )

    for r in range(len(cuts)):
        g_copy(r).start()
    open_line(0)
    for idx in order[:-1]:
        for i in range(2):
            plane_copy(idx, i).start()
    for idx in order[:-1]:
        q_copy(idx).start()

    half_way = len(steps) // 2
    for t in range(len(steps)):
        w_copy(t, True).wait()
        partial[t] = dot(own_g[...], own_w[t], NT)
        if t == half_way - 1:
            pass_plane(1)
    pass_plane(2)
    pass_plane(3)
    events = [(hops, idx) for hops in range(1, end) for idx in range(kv_heads)]
    slots = len(cuts) * len(steps) // 2
    done = 0
    for r, (start, size) in enumerate(cuts):
        rows = pl.ds(start, size)
        g_copy(r).wait_recv()
        for t, (idx, part) in enumerate(steps):
            if r == 0:
                w_copy(t, False).wait()
            block = partial[t, rows] + dot(other_g[rows], other_w[t], NT)
            u_buf[idx, rows, pl.ds(part * cut, cut)] = block.astype(jnp.bfloat16)
            if part == 1:
                if idx != 0:
                    u_copy(r, idx).start()
                at = r * len(steps) // 2 + t // 2 + 1
                while done < len(events) and done * slots < at * len(events):
                    pass_line(*events[done])
                    done += 1
    for hops, idx in events[done:]:
        pass_line(hops, idx)
    u_all[mine] = u_buf[0]

    for hops in range(1, planes):
        for idx in range(kv_heads):
            @pl.when(plane == end)
            def _():
                arrived(first + peers[idx] - hops * kv_heads)

            @pl.when(plane == 0)
            def _():
                arrived(first + peers[idx] + hops * kv_heads)

    for idx in order[:-1]:
        q_copy(idx).wait_recv()
        for r in range(len(cuts)):
            u_copy(r, idx).wait()
    for copy in own_copies:
        copy.wait()
    for r in range(len(cuts)):
        g_copy(r).wait_send()
    for idx in order[:-1]:
        q_copy(idx).wait_send()
        for i in range(2):
            plane_copy(idx, i).wait_send()
    for hops in range(end):
        for idx in range(kv_heads):
            for i in range(2):
                @pl.when((plane >= hops) & (plane < end))
                def _():
                    line_copy(0, hops, idx, i).wait_send()

                @pl.when((plane <= end - hops) & (plane > 0))
                def _():
                    line_copy(1, hops, idx, i).wait_send()


def score_kernel(
    order_ref, q_ref, k_ref, v_ref, u_ref, w_out, g_out, q_stack, u_stack,
    places, ks, vs, s_buf, p_buf,
):
    plane = lax.axis_index("cp") // q_ref.shape[0]
    own_rows = q_ref.shape[1]
    groups = q_ref.shape[2] // HEAD_DIM
    seq = k_ref.shape[0]
    spans = order_ref.shape[0]
    rows = seq // spans
    tile = groups * rows
    own_spans = q_ref.shape[0] * own_rows // rows
    per_block = own_rows // rows
    per_tile = TILE // rows
    scale = HEAD_DIM ** (-0.5) * 1.4426950408889634

    for r in range(spans):
        places[order_ref[r]] = r

    def place(j):
        return pl.ds(pl.multiple_of(places[j] * rows, rows), rows)

    for j in range(spans):
        for target, ref in ((ks, k_ref), (vs, v_ref)):
            target[pl.ds(j * rows, rows), :] = ref[place(j), :]

    def fold(x, op):
        return op(x.reshape(TILE // 8, 8, tile), axis=0)

    key_at = lax.broadcasted_iota(jnp.int32, (TILE, tile), 0)
    query_at = lax.rem(lax.broadcasted_iota(jnp.int32, (TILE, tile), 1), rows)

    def one_span(t, carry):
        block = t // per_block
        own = pl.ds(pl.multiple_of(lax.rem(t, per_block) * rows, rows), rows)
        cols = pl.ds(pl.multiple_of(t * tile, tile), tile)
        start = order_ref[plane * own_spans + t] * rows

        def stacked(ref):
            return jnp.concatenate(
                [ref[block, own, h * HEAD_DIM : (h + 1) * HEAD_DIM] for h in range(groups)], axis=0
            )

        def with_keys(last):
            q_tile = stacked(q_ref)
            u_tile = stacked(u_ref)
            q_stack[cols, :] = q_tile
            u_stack[cols, :] = u_tile
            peak = None
            for j in range(last + 1):
                keys = pl.ds(j * TILE, TILE)
                s = dot(ks[keys, :], q_tile, NT)
                if j == last:
                    s = jnp.where(key_at + (last * TILE - start) <= query_at, s, -1e30)
                s_buf[keys, :] = s
                top = fold(s, jnp.max)
                peak = top if peak is None else jnp.maximum(peak, top)
            peak = jnp.max(peak, axis=0, keepdims=True)
            total = jnp.zeros((8, tile), jnp.float32)
            delta = jnp.zeros((8, tile), jnp.float32)
            for j in range(last + 1):
                keys = pl.ds(j * TILE, TILE)
                p = jnp.exp2((s_buf[keys, :] - peak) * scale)
                dp = dot(vs[keys, :], u_tile, NT)
                total = total + fold(p, jnp.sum)
                delta = delta + fold(p * dp, jnp.sum)
                s_buf[keys, :] = p
                p_buf[keys, :] = dp
            inverse = 1.0 / jnp.sum(total, axis=0, keepdims=True)
            delta = jnp.sum(delta, axis=0, keepdims=True) * inverse
            for j in range(last + 1):
                keys = pl.ds(j * TILE, TILE)
                w = s_buf[keys, :] * inverse
                g = (w * (p_buf[keys, :] - delta)).astype(jnp.bfloat16)
                w = w.astype(jnp.bfloat16)
                for i in range(per_tile):
                    at = place(j * per_tile + i)
                    w_out[at, cols] = w[i * rows : (i + 1) * rows]
                    g_out[at, cols] = g[i * rows : (i + 1) * rows]
            blank = jnp.zeros((rows, tile), jnp.bfloat16)
            for j in range((last + 1) * per_tile, spans):
                w_out[place(j), cols] = blank
                g_out[place(j), cols] = blank

        for last in range(seq // TILE):
            pl.when(start // TILE == last)(functools.partial(with_keys, last))
        return carry

    lax.fori_loop(0, own_spans, one_span, 0)


def return_kernel(
    planes, kv_heads, w_ref, g_ref, q_ref, u_ref, k_ref, dq_all, dk_out, dv_out,
    k_turned, terms, summed, inbox, plane_box, dq_buf,
    send_sem, recv_sem, plane_sems, q_sems,
):
    me = lax.axis_index("cp")
    mine = lax.rem(me, kv_heads)
    plane = me // kv_heads
    first = plane * kv_heads
    end = planes - 1
    high = plane // 2
    outer = (plane == 0) | (plane == end)
    inner = 2 - high
    near = 1 + high
    peers = neighbours(mine)
    block_rows, wide = dq_buf.shape[1:]
    groups = wide // HEAD_DIM
    seq = g_ref.shape[0]
    tile = 2 * HEAD_DIM
    rows = tile // groups
    factor = HEAD_DIM ** (-0.5)

    for peer in peers[1:]:
        signal({"cp": first + peer})

    @pl.when(plane < end)
    def _():
        for m in range(kv_heads):
            signal({"cp": first + kv_heads + m})

    @pl.when(plane > 0)
    def _():
        for m in range(kv_heads):
            signal({"cp": first - kv_heads + m})

    def remote(source, target, sent, got, device):
        return pltpu.make_async_remote_copy(
            src_ref=source, dst_ref=target, send_sem=sent, recv_sem=got,
            device_id={"cp": device}, device_id_type=MESH,
        )

    def relay(source, stage, j, way, hops, device):
        slot = hops * kv_heads + j
        return remote(
            source, inbox.at[way, slot], send_sem.at[stage, j], recv_sem.at[way, slot],
            device * kv_heads + mine,
        )

    def final(source, stage, j, way, device):
        return remote(
            source, inbox.at[way, mine], send_sem.at[stage, j], recv_sem.at[way, mine],
            device * kv_heads + j,
        )

    def arrived(way, slot):
        at = inbox.at[way, slot]
        remote(at, at, send_sem.at[0, 0], recv_sem.at[way, slot], first + peers[1]).wait_recv()

    def chunk_of(i):
        return (1 - high) * (end - i) + high * i

    def compute(i):
        def one(j, carry):
            block = chunk_of(i) * kv_heads + j
            keys = pl.ds(pl.multiple_of(block * block_rows, block_rows), block_rows)
            dk = dot(g_ref[keys, :], q_ref[...], NN) * factor
            dv = dot(w_ref[keys, :], u_ref[...], NN)
            terms[block, :, :HEAD_DIM] = dk.astype(jnp.bfloat16)
            terms[block, :, HEAD_DIM:] = dv.astype(jnp.bfloat16)
            return carry

        lax.fori_loop(0, kv_heads, one, 0)

    def outward(i, j):
        source = terms.at[chunk_of(i) * kv_heads + j]
        if i == end - 1:
            return final(source, i, j, high, near)
        return relay(source, i, j, high, end - 1 - i, near)

    def plane_copy(idx):
        return remote(
            terms.at[first + peers[idx]], plane_box.at[mine],
            plane_sems.at[0, idx], plane_sems.at[1, mine], first + peers[idx],
        )

    def plane_arrived(idx):
        at = plane_box.at[peers[idx]]
        remote(at, at, plane_sems.at[0, idx], plane_sems.at[1, peers[idx]], first + peers[idx]).wait_recv()

    def dq_copy(idx):
        return remote(
            dq_buf.at[peers[idx]], columns(dq_all, mine, wide),
            q_sems.at[0, idx], q_sems.at[1, idx], first + peers[idx],
        )

    for i in range(planes):
        compute(i)
        if i == 0:
            lines = jnp.minimum(plane, 1) + jnp.minimum(end - plane, 1)
            pl.semaphore_wait(
                pltpu.get_barrier_semaphore(), kv_heads - 1 + kv_heads * lines
            )
        if i < end:
            @pl.when(outer)
            def _():
                for j in range(kv_heads):
                    outward(i, j).start()
    for idx in (2, 3, 1):
        plane_copy(idx).start()

    def middle(stage, way, slot, chunk, copy):
        for j in range(kv_heads):
            arrived(way, slot * kv_heads + j)
            total = terms[chunk * kv_heads + j].astype(jnp.float32) + inbox[
                way, slot * kv_heads + j
            ].astype(jnp.float32)
            summed[stage, j] = total.astype(jnp.bfloat16)
            copy(j).start()

    def onward(j):
        return relay(summed.at[0, j], 0, j, high, 1, inner)

    def to_end(j):
        return final(summed.at[1, j], 1, j, 1 - high, high * end)

    def to_inner(j):
        return final(summed.at[2, j], 2, j, high, inner)

    k_turned[...] = k_ref[...].T
    for t in range(seq // tile):
        cols = slice(t * tile, (t + 1) * tile)
        part = dot(k_turned[...], g_ref[:, cols], NN)
        part = (part.T * factor).astype(jnp.bfloat16)
        block, at = divmod(t * rows, block_rows)
        for h in range(groups):
            dq_buf[block, at : at + rows, h * HEAD_DIM : (h + 1) * HEAD_DIM] = part[
                h * rows : (h + 1) * rows
            ]
    for idx in (2, 3, 1):
        dq_copy(idx).start()

    @pl.when(jnp.logical_not(outer))
    def _():
        middle(0, high, 2, (1 - high) * end, onward)
        middle(1, 1 - high, 1, high * end, to_end)
        middle(2, high, 1, inner, to_inner)

    dq_all[:, pl.ds(pl.multiple_of(mine * wide, wide), wide)] = dq_buf[mine]
    plane_box[mine] = terms[me]

    def add(ref, m, value, fresh):
        cols = slice(m * HEAD_DIM, (m + 1) * HEAD_DIM)
        ref[:, cols] = value if fresh else ref[:, cols] + value

    def collect(box, m, fresh):
        value = box.astype(jnp.float32)
        add(dk_out, m, value[:, :HEAD_DIM], fresh)
        add(dv_out, m, value[:, HEAD_DIM:], fresh)

    for idx in range(1, kv_heads):
        plane_arrived(idx)
    for m in range(kv_heads):
        collect(plane_box[m], m, True)

    @pl.when(plane < end)
    def _():
        for m in range(kv_heads):
            arrived(1, m)
            collect(inbox[1, m], m, False)

    @pl.when(plane > 0)
    def _():
        for m in range(kv_heads):
            arrived(0, m)
            collect(inbox[0, m], m, False)

    for idx in range(1, kv_heads):
        plane_copy(idx).wait_send()
        dq_copy(idx).wait()

    @pl.when(outer)
    def _():
        for i in range(end):
            for j in range(kv_heads):
                outward(i, j).wait_send()

    @pl.when(jnp.logical_not(outer))
    def _():
        for copy in (onward, to_end, to_inner):
            for j in range(kv_heads):
                copy(j).wait_send()


def by_planes(n, queries, key_states, value_states, out_grad, o_weight, span_order):
    own_rows, width = queries.shape
    kv_heads = key_states.shape[1] // HEAD_DIM
    planes = n // kv_heads
    wide = width // kv_heads
    cut = wide // 2
    seq = own_rows * n
    tile = (HEADS // KV_HEADS) * (seq // span_order.shape[0])
    stack = kv_heads * own_rows * (HEADS // KV_HEADS)
    quarter = own_rows // 4
    cuts = ((0, 2 * quarter), (2 * quarter, quarter), (3 * quarter, quarter))
    any_spec = pl.BlockSpec(memory_space=pl.ANY)
    vmem_spec = pl.BlockSpec(memory_space=pltpu.VMEM)
    smem_spec = pl.BlockSpec(memory_space=pltpu.SMEM)
    dma = pltpu.SemaphoreType.DMA
    low = jnp.bfloat16
    q_block = pltpu.VMEM((kv_heads, own_rows, wide), low)
    kv_block = pltpu.VMEM((n, own_rows, HEAD_DIM), low)
    q_all, k_all, v_all, u_all = pl.pallas_call(
        functools.partial(send_kernel, planes, kv_heads, cuts),
        out_shape=(q_block, kv_block, kv_block, q_block),
        in_specs=[any_spec] * 5,
        out_specs=(vmem_spec,) * 4,
        scratch_shapes=[
            pltpu.VMEM((own_rows, width), low),
            pltpu.VMEM(key_states.shape, low),
            pltpu.VMEM(key_states.shape, low),
            pltpu.VMEM((own_rows, width), low),
            pltpu.VMEM((own_rows, width), low),
            pltpu.VMEM((2 * kv_heads, cut, width), low),
            pltpu.VMEM((2 * kv_heads, cut, width), low),
            pltpu.VMEM((2 * kv_heads, own_rows, cut), jnp.float32),
            pltpu.VMEM((kv_heads, own_rows, wide), low),
            dma((4,)),
            dma((3,)),
            dma((2, 2 * kv_heads)),
            dma((2, len(cuts))),
            dma((2, kv_heads)),
            dma((2, 2, (planes - 1) * kv_heads)),
            dma((2, n)),
            dma((2, kv_heads)),
            dma((2, len(cuts), kv_heads)),
        ],
        compiler_params=pltpu.CompilerParams(
            collective_id=0, has_side_effects=True, vmem_limit_bytes=SEND_LIMIT
        ),
        name="send_heads",
    )(queries, key_states, value_states, out_grad, o_weight)
    k_all = k_all.reshape(seq, HEAD_DIM)
    pair = jax.ShapeDtypeStruct((seq, stack), low)
    side = jax.ShapeDtypeStruct((stack, HEAD_DIM), low)
    weights, grads, q_stack, u_stack = pl.pallas_call(
        score_kernel,
        out_shape=(pair, pair, side, side),
        in_specs=[smem_spec] + [vmem_spec] * 4,
        out_specs=(vmem_spec,) * 4,
        scratch_shapes=[pltpu.SMEM(span_order.shape, jnp.int32)]
        + [pltpu.VMEM((seq, HEAD_DIM), low)] * 2
        + [pltpu.VMEM((seq, tile), jnp.float32)] * 2,
        compiler_params=pltpu.CompilerParams(vmem_limit_bytes=16 << 20),
        name="scores",
    )(span_order, q_all, k_all, v_all.reshape(seq, HEAD_DIM), u_all)
    term = (own_rows, 2 * HEAD_DIM)
    grad = jax.ShapeDtypeStruct(key_states.shape, jnp.float32)
    dq_all, key_grad, value_grad = pl.pallas_call(
        functools.partial(return_kernel, planes, kv_heads),
        out_shape=(jax.ShapeDtypeStruct((own_rows, width), low), grad, grad),
        in_specs=[vmem_spec] * 5,
        out_specs=(vmem_spec,) * 3,
        scratch_shapes=[
            pltpu.VMEM((HEAD_DIM, seq), low),
            pltpu.VMEM((n,) + term, low),
            pltpu.VMEM((3, kv_heads) + term, low),
            pltpu.VMEM((2, 3 * kv_heads) + term, low),
            pltpu.VMEM((kv_heads,) + term, low),
            pltpu.VMEM((kv_heads, own_rows, wide), low),
            dma((3, kv_heads)),
            dma((2, 3 * kv_heads)),
            dma((2, kv_heads)),
            dma((2, kv_heads)),
        ],
        compiler_params=pltpu.CompilerParams(
            collective_id=1, has_side_effects=True, vmem_limit_bytes=16 << 20
        ),
        name="return_grads",
    )(weights, grads, q_stack, u_stack, k_all)
    return (dq_all.astype(jnp.float32), key_grad, value_grad)


SEND_LIMIT = 60 << 20


def solution(mesh):
    n = mesh.shape["cp"]
    planes = mesh.shape["vocab"] == 2 and n == 4 * (KV_HEADS // 2)
    body = functools.partial(by_planes, n) if planes else local
    return jax.shard_map(
        body,
        mesh=mesh,
        in_specs=(
            P("cp", "vocab"),
            P("cp", "vocab"),
            P("cp", "vocab"),
            P("cp", "vocab"),
            P("vocab", None),
            P(),
        ),
        out_specs=(P("cp", "vocab"), P("cp", "vocab"), P("cp", "vocab")),
        check_vma=False,
    )
```

```python
import functools

import jax
import jax.numpy as jnp
from jax import lax
from jax.experimental import pallas as pl
from jax.experimental.pallas import tpu as pltpu
from jax.sharding import PartitionSpec as P

HEADS = 32
KV_HEADS = 8
HEAD_DIM = 128


def positions(span_order, span_rows):
    offsets = jnp.arange(span_rows, dtype=jnp.int32)
    return (span_order[:, None] * span_rows + offsets[None, :]).reshape(-1)


def block_scores(query_block, key_block, query_places, key_places, factor):
    scores = (
        jnp.einsum("qkgd,skd->kgqs", query_block, key_block, preferred_element_type=jnp.float32)
        * factor
    )
    visible = key_places[None, :] <= query_places[:, None]
    return jnp.where(visible, scores, -jnp.inf)


def local(queries, key_states, value_states, out_grad, o_weight, span_order):
    own_rows = queries.shape[0]
    kv_width = key_states.shape[1]
    kv_heads = kv_width // HEAD_DIM
    groups = HEADS // KV_HEADS
    factor = HEAD_DIM ** (-0.5)
    upstream = lax.dot_general(
        lax.all_gather(out_grad, "vocab", axis=1, tiled=True),
        o_weight,
        (((1,), (1,)), ((), ())),
        preferred_element_type=jnp.float32,
    ).astype(jnp.bfloat16)
    places = positions(span_order, own_rows // 2)
    seq_len = places.shape[0]
    own_places = lax.dynamic_slice_in_dim(places, lax.axis_index("cp") * own_rows, own_rows, 0)
    query_heads = queries.reshape(own_rows, kv_heads, groups, HEAD_DIM)
    upstream_heads = upstream.reshape(own_rows, kv_heads, groups, HEAD_DIM)
    key_all, value_all = (
        lax.all_gather(key_states, "cp", axis=0, tiled=True),
        lax.all_gather(value_states, "cp", axis=0, tiled=True),
    )
    key_all = key_all.reshape(seq_len, kv_heads, HEAD_DIM)
    value_all = value_all.reshape(seq_len, kv_heads, HEAD_DIM)
    block_rows = own_rows * 8
    block_count = seq_len // block_rows
    block_ids = jnp.arange(block_count, dtype=jnp.int32)
    stat_shape = (kv_heads, groups, own_rows)

    def key_block(block_index):
        offset = block_index * block_rows
        return (
            lax.dynamic_slice_in_dim(key_all, offset, block_rows, 0),
            lax.dynamic_slice_in_dim(value_all, offset, block_rows, 0),
            lax.dynamic_slice_in_dim(places, offset, block_rows, 0),
        )

    def stats_step(carried, block_index):
        running, totals, delta_acc = carried
        keys_now, values_now, places_now = key_block(block_index)
        scores = block_scores(query_heads, keys_now, own_places, places_now, factor)
        newest = jnp.maximum(running, jnp.max(scores, axis=3))
        rescale = jnp.exp(running - newest)
        raised = jnp.exp(scores - newest[..., None])
        grad_probs = jnp.einsum(
            "qkgd,skd->kgqs", upstream_heads, values_now, preferred_element_type=jnp.float32
        )
        totals = totals * rescale + jnp.sum(raised, axis=3)
        delta_acc = delta_acc * rescale + jnp.sum(raised * grad_probs, axis=3)
        return ((newest, totals, delta_acc), None)

    start_stats = (
        jnp.full(stat_shape, -1e30, jnp.float32),
        jnp.zeros(stat_shape, jnp.float32),
        jnp.zeros(stat_shape, jnp.float32),
    )
    (running, totals, delta_acc), unused = lax.scan(stats_step, start_stats, block_ids)
    logsum = running + jnp.log(totals)
    deltas = delta_acc / totals

    def grad_pieces(block_index):
        keys_now, values_now, places_now = key_block(block_index)
        scores = block_scores(query_heads, keys_now, own_places, places_now, factor)
        weights = jnp.exp(scores - logsum[..., None])
        grad_probs = jnp.einsum(
            "qkgd,skd->kgqs", upstream_heads, values_now, preferred_element_type=jnp.float32
        )
        grad_scores = (weights * (grad_probs - deltas[..., None])).astype(jnp.bfloat16)
        return (keys_now, weights, grad_scores)

    query_zeros = jnp.zeros((own_rows, kv_heads, groups, HEAD_DIM), jnp.float32)

    def grad_step(carried, block_index):
        keys_now, weights, grad_scores = grad_pieces(block_index)
        carried = (
            carried
            + jnp.einsum(
                "kgqs,skd->qkgd", grad_scores, keys_now, preferred_element_type=jnp.float32
            )
            * factor
        )
        key_term = (
            jnp.einsum(
                "kgqs,qkgd->skd", grad_scores, query_heads, preferred_element_type=jnp.float32
            )
            * factor
        )
        value_term = jnp.einsum(
            "kgqs,qkgd->skd",
            weights.astype(jnp.bfloat16),
            upstream_heads,
            preferred_element_type=jnp.float32,
        )
        joined = jnp.concatenate(
            (key_term.reshape(block_rows, kv_width), value_term.reshape(block_rows, kv_width)),
            axis=1,
        )
        return (carried, joined)

    query_total, stacked = lax.scan(grad_step, query_zeros, block_ids)
    terms = stacked.reshape(seq_len, 2 * kv_width)
    mine = lax.psum_scatter(
        terms.astype(jnp.bfloat16), "cp", scatter_dimension=0, tiled=True
    ).astype(jnp.float32)
    key_grad = mine[:, :kv_width]
    value_grad = mine[:, kv_width:]
    query_grad = query_total.reshape(own_rows, kv_heads * groups * HEAD_DIM)
    return (query_grad, key_grad, value_grad)


MESH = pl.DeviceIdType.MESH
NT = (((1,), (1,)), ((), ()))
NN = (((1,), (0,)), ((), ()))
TILE = 256


def dot(a, b, dims):
    return lax.dot_general(a, b, dims, preferred_element_type=jnp.float32)


def neighbours(mine):
    partner = mine + 1 - 2 * lax.rem(mine, 2)
    return [mine, partner, lax.rem(mine + 2, 4), lax.rem(partner + 2, 4)]


def signal(peer):
    pl.semaphore_signal(
        pltpu.get_barrier_semaphore(), inc=1, device_id=peer, device_id_type=MESH
    )


def columns(ref, at, size):
    return ref.at[:, pl.ds(pl.multiple_of(at * size, size), size)]


def send_kernel(
    planes, kv_heads, cuts, q_ref, k_ref, v_ref, g_ref, w_ref, q_all, k_all, v_all, u_all,
    own_q, own_k, own_v, own_g, other_g, own_w, other_w, partial, u_buf,
    load_sem, own_sem, w_sem, g_sem, plane_sem, line_sem, kv_sem, q_sems, u_sems,
):
    me = lax.axis_index("cp")
    half = lax.axis_index("vocab")
    mine = lax.rem(me, kv_heads)
    plane = me // kv_heads
    first = plane * kv_heads
    end = planes - 1
    width = g_ref.shape[1]
    wide = width // kv_heads
    cut = wide // 2
    peers = neighbours(mine)
    order = [2, 3, 1, 0]
    steps = [(idx, part) for idx in order for part in range(2)]

    def w_copy(t, own):
        idx, part = steps[t]
        side = half if own else 1 - half
        return pltpu.make_async_copy(
            w_ref.at[
                pl.ds(pl.multiple_of(peers[idx] * wide + part * cut, cut), cut),
                pl.ds(pl.multiple_of(side * width, width), width),
            ],
            (own_w if own else other_w).at[t],
            w_sem.at[0 if own else 1, t],
        )

    loads = [
        pltpu.make_async_copy(source, target, load_sem.at[i])
        for i, (source, target) in enumerate(
            ((g_ref, own_g), (k_ref, own_k), (v_ref, own_v), (q_ref, own_q))
        )
    ]
    for copy in loads:
        copy.start()
    own_copies = [
        pltpu.make_async_copy(columns(q_ref, mine, wide), q_all.at[mine], own_sem.at[0]),
        pltpu.make_async_copy(columns(k_ref, mine, HEAD_DIM), k_all.at[me], own_sem.at[1]),
        pltpu.make_async_copy(columns(v_ref, mine, HEAD_DIM), v_all.at[me], own_sem.at[2]),
    ]
    for copy in own_copies:
        copy.start()
    signal({"vocab": 1 - half})
    for peer in peers[1:]:
        signal({"cp": first + peer})

    @pl.when(plane < end)
    def _():
        signal({"cp": me + kv_heads})

    @pl.when(plane > 0)
    def _():
        signal({"cp": me - kv_heads})

    lines = jnp.minimum(plane, 1) + jnp.minimum(end - plane, 1)
    for copy in loads:
        copy.wait()
    for own in (True, False):
        for t in range(len(steps)):
            w_copy(t, own).start()
    pl.semaphore_wait(pltpu.get_barrier_semaphore(), kv_heads + lines)

    def g_copy(r):
        rows = pl.ds(*cuts[r])
        return pltpu.make_async_remote_copy(
            src_ref=own_g.at[rows], dst_ref=other_g.at[rows],
            send_sem=g_sem.at[0, r], recv_sem=g_sem.at[1, r],
            device_id={"vocab": 1 - half}, device_id_type=MESH,
        )

    def plane_copy(idx, i):
        return pltpu.make_async_remote_copy(
            src_ref=columns((own_k, own_v)[i], peers[idx], HEAD_DIM),
            dst_ref=(k_all, v_all)[i].at[me],
            send_sem=plane_sem.at[i, idx], recv_sem=kv_sem.at[i, me],
            device_id={"cp": first + peers[idx]}, device_id_type=MESH,
        )

    def line_copy(left, hops, idx, i):
        block = me - mine + peers[idx] + (kv_heads if left else -kv_heads) * hops
        kept = (k_all, v_all)[i]
        own = hops == 0 and idx == 0
        return pltpu.make_async_remote_copy(
            src_ref=columns((own_k, own_v)[i], mine, HEAD_DIM) if own else kept.at[block],
            dst_ref=kept.at[block],
            send_sem=line_sem.at[left, i, hops * kv_heads + idx], recv_sem=kv_sem.at[i, block],
            device_id={"cp": me + (-kv_heads if left else kv_heads)}, device_id_type=MESH,
        )

    def arrived(block):
        for i in range(2):
            slot = (k_all, v_all)[i].at[block]
            pltpu.make_async_remote_copy(
                src_ref=slot, dst_ref=slot,
                send_sem=plane_sem.at[i, 0], recv_sem=kv_sem.at[i, block],
                device_id={"cp": first + peers[1]}, device_id_type=MESH,
            ).wait_recv()

    def start_line(left, hops, idx):
        for i in range(2):
            line_copy(left, hops, idx, i).start()

    def open_line(idx):
        @pl.when(plane < end)
        def _():
            start_line(0, 0, idx)

        @pl.when(plane > 0)
        def _():
            start_line(1, 0, idx)

    def pass_plane(idx):
        arrived(first + peers[idx])
        open_line(idx)

    def pass_line(hops, idx):
        @pl.when((plane >= hops) & (plane < end))
        def _():
            arrived(first + peers[idx] - hops * kv_heads)
            start_line(0, hops, idx)

        @pl.when((plane <= end - hops) & (plane > 0))
        def _():
            arrived(first + peers[idx] + hops * kv_heads)
            start_line(1, hops, idx)

    def q_copy(idx):
        return pltpu.make_async_remote_copy(
            src_ref=columns(own_q, peers[idx], wide), dst_ref=q_all.at[mine],
            send_sem=q_sems.at[0, idx], recv_sem=q_sems.at[1, idx],
            device_id={"cp": first + peers[idx]}, device_id_type=MESH,
        )

    def u_copy(r, idx):
        rows = pl.ds(*cuts[r])
        return pltpu.make_async_remote_copy(
            src_ref=u_buf.at[idx, rows], dst_ref=u_all.at[mine, rows],
            send_sem=u_sems.at[0, r, idx], recv_sem=u_sems.at[1, r, idx],
            device_id={"cp": first + peers[idx]}, device_id_type=MESH,
        )

    for r in range(len(cuts)):
        g_copy(r).start()
    open_line(0)
    for idx in order[:-1]:
        for i in range(2):
            plane_copy(idx, i).start()
    for idx in order[:-1]:
        q_copy(idx).start()

    half_way = len(steps) // 2
    for t in range(len(steps)):
        w_copy(t, True).wait()
        partial[t] = dot(own_g[...], own_w[t], NT)
        if t == half_way - 1:
            pass_plane(1)
    pass_plane(2)
    pass_plane(3)
    events = [(hops, idx) for hops in range(1, end) for idx in range(kv_heads)]
    done = kv_heads - 1
    for hops, idx in events[:done]:
        pass_line(hops, idx)
    for r, (start, size) in enumerate(cuts):
        rows = pl.ds(start, size)
        g_copy(r).wait_recv()
        for t, (idx, part) in enumerate(steps):
            if r == 0:
                w_copy(t, False).wait()
            block = partial[t, rows] + dot(other_g[rows], other_w[t], NT)
            u_buf[idx, rows, pl.ds(part * cut, cut)] = block.astype(jnp.bfloat16)
            if part == 1:
                if idx != 0:
                    u_copy(r, idx).start()
                if True and done < len(events):
                    pass_line(*events[done])
                    done += 1
    for hops, idx in events[done:]:
        pass_line(hops, idx)
    u_all[mine] = u_buf[0]

    for hops in range(1, planes):
        for idx in range(kv_heads):
            @pl.when(plane == end)
            def _():
                arrived(first + peers[idx] - hops * kv_heads)

            @pl.when(plane == 0)
            def _():
                arrived(first + peers[idx] + hops * kv_heads)

    for idx in order[:-1]:
        q_copy(idx).wait_recv()
        for r in range(len(cuts)):
            u_copy(r, idx).wait()
    for copy in own_copies:
        copy.wait()
    for r in range(len(cuts)):
        g_copy(r).wait_send()
    for idx in order[:-1]:
        q_copy(idx).wait_send()
        for i in range(2):
            plane_copy(idx, i).wait_send()
    for hops in range(end):
        for idx in range(kv_heads):
            for i in range(2):
                @pl.when((plane >= hops) & (plane < end))
                def _():
                    line_copy(0, hops, idx, i).wait_send()

                @pl.when((plane <= end - hops) & (plane > 0))
                def _():
                    line_copy(1, hops, idx, i).wait_send()


def score_kernel(
    order_ref, q_ref, k_ref, v_ref, u_ref, w_out, g_out, q_stack, u_stack,
    places, ks, vs, s_buf, p_buf,
):
    plane = lax.axis_index("cp") // q_ref.shape[0]
    own_rows = q_ref.shape[1]
    groups = q_ref.shape[2] // HEAD_DIM
    seq = k_ref.shape[0]
    spans = order_ref.shape[0]
    rows = seq // spans
    tile = groups * rows
    own_spans = q_ref.shape[0] * own_rows // rows
    per_block = own_rows // rows
    per_tile = TILE // rows
    scale = HEAD_DIM ** (-0.5) * 1.4426950408889634

    for r in range(spans):
        places[order_ref[r]] = r

    def place(j):
        return pl.ds(pl.multiple_of(places[j] * rows, rows), rows)

    for j in range(spans):
        for target, ref in ((ks, k_ref), (vs, v_ref)):
            target[pl.ds(j * rows, rows), :] = ref[place(j), :]

    def fold(x, op):
        return op(x.reshape(TILE // 8, 8, tile), axis=0)

    key_at = lax.broadcasted_iota(jnp.int32, (TILE, tile), 0)
    query_at = lax.rem(lax.broadcasted_iota(jnp.int32, (TILE, tile), 1), rows)

    def one_span(t, carry):
        block = t // per_block
        own = pl.ds(pl.multiple_of(lax.rem(t, per_block) * rows, rows), rows)
        cols = pl.ds(pl.multiple_of(t * tile, tile), tile)
        start = order_ref[plane * own_spans + t] * rows

        def stacked(ref):
            return jnp.concatenate(
                [ref[block, own, h * HEAD_DIM : (h + 1) * HEAD_DIM] for h in range(groups)], axis=0
            )

        def with_keys(last):
            q_tile = stacked(q_ref)
            u_tile = stacked(u_ref)
            q_stack[cols, :] = q_tile
            u_stack[cols, :] = u_tile
            peak = None
            for j in range(last + 1):
                keys = pl.ds(j * TILE, TILE)
                s = dot(ks[keys, :], q_tile, NT)
                if j == last:
                    s = jnp.where(key_at + (last * TILE - start) <= query_at, s, -1e30)
                s_buf[keys, :] = s
                top = fold(s, jnp.max)
                peak = top if peak is None else jnp.maximum(peak, top)
            peak = jnp.max(peak, axis=0, keepdims=True)
            total = jnp.zeros((8, tile), jnp.float32)
            delta = jnp.zeros((8, tile), jnp.float32)
            for j in range(last + 1):
                keys = pl.ds(j * TILE, TILE)
                p = jnp.exp2((s_buf[keys, :] - peak) * scale)
                dp = dot(vs[keys, :], u_tile, NT)
                total = total + fold(p, jnp.sum)
                delta = delta + fold(p * dp, jnp.sum)
                s_buf[keys, :] = p
                p_buf[keys, :] = dp
            inverse = 1.0 / jnp.sum(total, axis=0, keepdims=True)
            delta = jnp.sum(delta, axis=0, keepdims=True) * inverse
            for j in range(last + 1):
                keys = pl.ds(j * TILE, TILE)
                w = s_buf[keys, :] * inverse
                g = (w * (p_buf[keys, :] - delta)).astype(jnp.bfloat16)
                w = w.astype(jnp.bfloat16)
                for i in range(per_tile):
                    at = place(j * per_tile + i)
                    w_out[at, cols] = w[i * rows : (i + 1) * rows]
                    g_out[at, cols] = g[i * rows : (i + 1) * rows]
            blank = jnp.zeros((rows, tile), jnp.bfloat16)
            for j in range((last + 1) * per_tile, spans):
                w_out[place(j), cols] = blank
                g_out[place(j), cols] = blank

        for last in range(seq // TILE):
            pl.when(start // TILE == last)(functools.partial(with_keys, last))
        return carry

    lax.fori_loop(0, own_spans, one_span, 0)


def return_kernel(
    planes, kv_heads, w_ref, g_ref, q_ref, u_ref, k_ref, dq_all, dk_out, dv_out,
    k_turned, terms, summed, inbox, plane_box, dq_buf,
    send_sem, recv_sem, plane_sems, q_sems,
):
    me = lax.axis_index("cp")
    mine = lax.rem(me, kv_heads)
    plane = me // kv_heads
    first = plane * kv_heads
    end = planes - 1
    high = plane // 2
    outer = (plane == 0) | (plane == end)
    inner = 2 - high
    near = 1 + high
    peers = neighbours(mine)
    block_rows, wide = dq_buf.shape[1:]
    groups = wide // HEAD_DIM
    seq = g_ref.shape[0]
    tile = 2 * HEAD_DIM
    rows = tile // groups
    factor = HEAD_DIM ** (-0.5)

    for peer in peers[1:]:
        signal({"cp": first + peer})

    @pl.when(plane < end)
    def _():
        for m in range(kv_heads):
            signal({"cp": first + kv_heads + m})

    @pl.when(plane > 0)
    def _():
        for m in range(kv_heads):
            signal({"cp": first - kv_heads + m})

    def remote(source, target, sent, got, device):
        return pltpu.make_async_remote_copy(
            src_ref=source, dst_ref=target, send_sem=sent, recv_sem=got,
            device_id={"cp": device}, device_id_type=MESH,
        )

    def relay(source, stage, j, way, hops, device):
        slot = hops * kv_heads + j
        return remote(
            source, inbox.at[way, slot], send_sem.at[stage, j], recv_sem.at[way, slot],
            device * kv_heads + mine,
        )

    def final(source, stage, j, way, device):
        return remote(
            source, inbox.at[way, mine], send_sem.at[stage, j], recv_sem.at[way, mine],
            device * kv_heads + j,
        )

    def arrived(way, slot):
        at = inbox.at[way, slot]
        remote(at, at, send_sem.at[0, 0], recv_sem.at[way, slot], first + peers[1]).wait_recv()

    def chunk_of(i):
        return (1 - high) * (end - i) + high * i

    def compute(i):
        def one(j, carry):
            block = chunk_of(i) * kv_heads + j
            keys = pl.ds(pl.multiple_of(block * block_rows, block_rows), block_rows)
            dk = dot(g_ref[keys, :], q_ref[...], NN) * factor
            dv = dot(w_ref[keys, :], u_ref[...], NN)
            terms[block, :, :HEAD_DIM] = dk.astype(jnp.bfloat16)
            terms[block, :, HEAD_DIM:] = dv.astype(jnp.bfloat16)
            return carry

        lax.fori_loop(0, kv_heads, one, 0)

    def outward(i, j):
        source = terms.at[chunk_of(i) * kv_heads + j]
        if i == end - 1:
            return final(source, i, j, high, near)
        return relay(source, i, j, high, end - 1 - i, near)

    def plane_copy(idx):
        return remote(
            terms.at[first + peers[idx]], plane_box.at[mine],
            plane_sems.at[0, idx], plane_sems.at[1, mine], first + peers[idx],
        )

    def plane_arrived(idx):
        at = plane_box.at[peers[idx]]
        remote(at, at, plane_sems.at[0, idx], plane_sems.at[1, peers[idx]], first + peers[idx]).wait_recv()

    def dq_copy(idx):
        return remote(
            dq_buf.at[peers[idx]], columns(dq_all, mine, wide),
            q_sems.at[0, idx], q_sems.at[1, idx], first + peers[idx],
        )

    for i in range(planes):
        compute(i)
        if i == 0:
            lines = jnp.minimum(plane, 1) + jnp.minimum(end - plane, 1)
            pl.semaphore_wait(
                pltpu.get_barrier_semaphore(), kv_heads - 1 + kv_heads * lines
            )
        if i < end:
            @pl.when(outer)
            def _():
                for j in range(kv_heads):
                    outward(i, j).start()
    for idx in (2, 3, 1):
        plane_copy(idx).start()

    def middle(stage, way, slot, chunk, copy):
        for j in range(kv_heads):
            arrived(way, slot * kv_heads + j)
            total = terms[chunk * kv_heads + j].astype(jnp.float32) + inbox[
                way, slot * kv_heads + j
            ].astype(jnp.float32)
            summed[stage, j] = total.astype(jnp.bfloat16)
            copy(j).start()

    def onward(j):
        return relay(summed.at[0, j], 0, j, high, 1, inner)

    def to_end(j):
        return final(summed.at[1, j], 1, j, 1 - high, high * end)

    def to_inner(j):
        return final(summed.at[2, j], 2, j, high, inner)

    k_turned[...] = k_ref[...].T
    for t in range(seq // tile):
        cols = slice(t * tile, (t + 1) * tile)
        part = dot(k_turned[...], g_ref[:, cols], NN)
        part = (part.T * factor).astype(jnp.bfloat16)
        block, at = divmod(t * rows, block_rows)
        for h in range(groups):
            dq_buf[block, at : at + rows, h * HEAD_DIM : (h + 1) * HEAD_DIM] = part[
                h * rows : (h + 1) * rows
            ]
    for idx in (2, 3, 1):
        dq_copy(idx).start()

    @pl.when(jnp.logical_not(outer))
    def _():
        middle(0, high, 2, (1 - high) * end, onward)
        middle(1, 1 - high, 1, high * end, to_end)
        middle(2, high, 1, inner, to_inner)

    dq_all[:, pl.ds(pl.multiple_of(mine * wide, wide), wide)] = dq_buf[mine]
    plane_box[mine] = terms[me]

    def add(ref, m, value, fresh):
        cols = slice(m * HEAD_DIM, (m + 1) * HEAD_DIM)
        ref[:, cols] = value if fresh else ref[:, cols] + value

    def collect(box, m, fresh):
        value = box.astype(jnp.float32)
        add(dk_out, m, value[:, :HEAD_DIM], fresh)
        add(dv_out, m, value[:, HEAD_DIM:], fresh)

    for idx in range(1, kv_heads):
        plane_arrived(idx)
    for m in range(kv_heads):
        collect(plane_box[m], m, True)

    @pl.when(plane < end)
    def _():
        for m in range(kv_heads):
            arrived(1, m)
            collect(inbox[1, m], m, False)

    @pl.when(plane > 0)
    def _():
        for m in range(kv_heads):
            arrived(0, m)
            collect(inbox[0, m], m, False)

    for idx in range(1, kv_heads):
        plane_copy(idx).wait_send()
        dq_copy(idx).wait()

    @pl.when(outer)
    def _():
        for i in range(end):
            for j in range(kv_heads):
                outward(i, j).wait_send()

    @pl.when(jnp.logical_not(outer))
    def _():
        for copy in (onward, to_end, to_inner):
            for j in range(kv_heads):
                copy(j).wait_send()


def finish_kernel(dq_ref, dk_ref, dv_ref, dq_out, dk_out, dv_out, wide, sems):
    parts = wide.shape[0]
    rows = wide.shape[1]
    copies = [
        pltpu.make_async_copy(dk_ref, dk_out, sems.at[parts]),
        pltpu.make_async_copy(dv_ref, dv_out, sems.at[parts + 1]),
    ]
    for copy in copies:
        copy.start()
    for i in range(parts):
        at = pl.ds(i * rows, rows)
        wide[i] = dq_ref[at, :].astype(jnp.float32)
        copy = pltpu.make_async_copy(wide.at[i], dq_out.at[at], sems.at[i])
        copy.start()
        copies.append(copy)
    for copy in copies:
        copy.wait()


def by_planes(n, queries, key_states, value_states, out_grad, o_weight, span_order):
    own_rows, width = queries.shape
    kv_heads = key_states.shape[1] // HEAD_DIM
    planes = n // kv_heads
    wide = width // kv_heads
    cut = wide // 2
    seq = own_rows * n
    tile = (HEADS // KV_HEADS) * (seq // span_order.shape[0])
    stack = kv_heads * own_rows * (HEADS // KV_HEADS)
    quarter = own_rows // 4
    cuts = ((0, 2 * quarter), (2 * quarter, 2 * quarter))
    any_spec = pl.BlockSpec(memory_space=pl.ANY)
    vmem_spec = pl.BlockSpec(memory_space=pltpu.VMEM)
    smem_spec = pl.BlockSpec(memory_space=pltpu.SMEM)
    dma = pltpu.SemaphoreType.DMA
    low = jnp.bfloat16
    q_block = pltpu.VMEM((kv_heads, own_rows, wide), low)
    kv_block = pltpu.VMEM((n, own_rows, HEAD_DIM), low)
    q_all, k_all, v_all, u_all = pl.pallas_call(
        functools.partial(send_kernel, planes, kv_heads, cuts),
        out_shape=(q_block, kv_block, kv_block, q_block),
        in_specs=[any_spec] * 5,
        out_specs=(vmem_spec,) * 4,
        scratch_shapes=[
            pltpu.VMEM((own_rows, width), low),
            pltpu.VMEM(key_states.shape, low),
            pltpu.VMEM(key_states.shape, low),
            pltpu.VMEM((own_rows, width), low),
            pltpu.VMEM((own_rows, width), low),
            pltpu.VMEM((2 * kv_heads, cut, width), low),
            pltpu.VMEM((2 * kv_heads, cut, width), low),
            pltpu.VMEM((2 * kv_heads, own_rows, cut), jnp.float32),
            pltpu.VMEM((kv_heads, own_rows, wide), low),
            dma((4,)),
            dma((3,)),
            dma((2, 2 * kv_heads)),
            dma((2, len(cuts))),
            dma((2, kv_heads)),
            dma((2, 2, (planes - 1) * kv_heads)),
            dma((2, n)),
            dma((2, kv_heads)),
            dma((2, len(cuts), kv_heads)),
        ],
        compiler_params=pltpu.CompilerParams(
            collective_id=0, has_side_effects=True, vmem_limit_bytes=SEND_LIMIT
        ),
        name="send_heads",
    )(queries, key_states, value_states, out_grad, o_weight)
    k_all = k_all.reshape(seq, HEAD_DIM)
    pair = jax.ShapeDtypeStruct((seq, stack), low)
    side = jax.ShapeDtypeStruct((stack, HEAD_DIM), low)
    weights, grads, q_stack, u_stack = pl.pallas_call(
        score_kernel,
        out_shape=(pair, pair, side, side),
        in_specs=[smem_spec] + [vmem_spec] * 4,
        out_specs=(vmem_spec,) * 4,
        scratch_shapes=[pltpu.SMEM(span_order.shape, jnp.int32)]
        + [pltpu.VMEM((seq, HEAD_DIM), low)] * 2
        + [pltpu.VMEM((seq, tile), jnp.float32)] * 2,
        compiler_params=pltpu.CompilerParams(vmem_limit_bytes=16 << 20),
        name="scores",
    )(span_order, q_all, k_all, v_all.reshape(seq, HEAD_DIM), u_all)
    term = (own_rows, 2 * HEAD_DIM)
    grad = jax.ShapeDtypeStruct(key_states.shape, jnp.float32)
    dq_all, key_grad, value_grad = pl.pallas_call(
        functools.partial(return_kernel, planes, kv_heads),
        out_shape=(jax.ShapeDtypeStruct((own_rows, width), low), grad, grad),
        in_specs=[vmem_spec] * 5,
        out_specs=(vmem_spec,) * 3,
        scratch_shapes=[
            pltpu.VMEM((HEAD_DIM, seq), low),
            pltpu.VMEM((n,) + term, low),
            pltpu.VMEM((3, kv_heads) + term, low),
            pltpu.VMEM((2, 3 * kv_heads) + term, low),
            pltpu.VMEM((kv_heads,) + term, low),
            pltpu.VMEM((kv_heads, own_rows, wide), low),
            dma((3, kv_heads)),
            dma((2, 3 * kv_heads)),
            dma((2, kv_heads)),
            dma((2, kv_heads)),
        ],
        compiler_params=pltpu.CompilerParams(
            collective_id=1, has_side_effects=True, vmem_limit_bytes=16 << 20
        ),
        name="return_grads",
    )(weights, grads, q_stack, u_stack, k_all)
    parts = 8
    return pl.pallas_call(
        finish_kernel,
        out_shape=(jax.ShapeDtypeStruct(queries.shape, jnp.float32), grad, grad),
        in_specs=[vmem_spec] * 3,
        out_specs=(any_spec,) * 3,
        scratch_shapes=[
            pltpu.VMEM((parts, own_rows // parts, width), jnp.float32),
            dma((parts + 2,)),
        ],
        compiler_params=pltpu.CompilerParams(vmem_limit_bytes=8 << 20),
        name="finish",
    )(dq_all, key_grad, value_grad)


SEND_LIMIT = 60 << 20


def solution(mesh):
    n = mesh.shape["cp"]
    planes = mesh.shape["vocab"] == 2 and n == 4 * (KV_HEADS // 2)
    body = functools.partial(by_planes, n) if planes else local
    return jax.shard_map(
        body,
        mesh=mesh,
        in_specs=(
            P("cp", "vocab"),
            P("cp", "vocab"),
            P("cp", "vocab"),
            P("cp", "vocab"),
            P("vocab", None),
            P(),
        ),
        out_specs=(P("cp", "vocab"), P("cp", "vocab"), P("cp", "vocab")),
        check_vma=False,
    )
```

```python
import functools

import jax
import jax.numpy as jnp
from jax import lax
from jax.experimental import pallas as pl
from jax.experimental.pallas import tpu as pltpu
from jax.sharding import PartitionSpec as P

HEADS = 32
KV_HEADS = 8
HEAD_DIM = 128


def positions(span_order, span_rows):
    offsets = jnp.arange(span_rows, dtype=jnp.int32)
    return (span_order[:, None] * span_rows + offsets[None, :]).reshape(-1)


def block_scores(query_block, key_block, query_places, key_places, factor):
    scores = (
        jnp.einsum("qkgd,skd->kgqs", query_block, key_block, preferred_element_type=jnp.float32)
        * factor
    )
    visible = key_places[None, :] <= query_places[:, None]
    return jnp.where(visible, scores, -jnp.inf)


def local(queries, key_states, value_states, out_grad, o_weight, span_order):
    own_rows = queries.shape[0]
    kv_width = key_states.shape[1]
    kv_heads = kv_width // HEAD_DIM
    groups = HEADS // KV_HEADS
    factor = HEAD_DIM ** (-0.5)
    upstream = lax.dot_general(
        lax.all_gather(out_grad, "vocab", axis=1, tiled=True),
        o_weight,
        (((1,), (1,)), ((), ())),
        preferred_element_type=jnp.float32,
    ).astype(jnp.bfloat16)
    places = positions(span_order, own_rows // 2)
    seq_len = places.shape[0]
    own_places = lax.dynamic_slice_in_dim(places, lax.axis_index("cp") * own_rows, own_rows, 0)
    query_heads = queries.reshape(own_rows, kv_heads, groups, HEAD_DIM)
    upstream_heads = upstream.reshape(own_rows, kv_heads, groups, HEAD_DIM)
    key_all, value_all = (
        lax.all_gather(key_states, "cp", axis=0, tiled=True),
        lax.all_gather(value_states, "cp", axis=0, tiled=True),
    )
    key_all = key_all.reshape(seq_len, kv_heads, HEAD_DIM)
    value_all = value_all.reshape(seq_len, kv_heads, HEAD_DIM)
    block_rows = own_rows * 8
    block_count = seq_len // block_rows
    block_ids = jnp.arange(block_count, dtype=jnp.int32)
    stat_shape = (kv_heads, groups, own_rows)

    def key_block(block_index):
        offset = block_index * block_rows
        return (
            lax.dynamic_slice_in_dim(key_all, offset, block_rows, 0),
            lax.dynamic_slice_in_dim(value_all, offset, block_rows, 0),
            lax.dynamic_slice_in_dim(places, offset, block_rows, 0),
        )

    def stats_step(carried, block_index):
        running, totals, delta_acc = carried
        keys_now, values_now, places_now = key_block(block_index)
        scores = block_scores(query_heads, keys_now, own_places, places_now, factor)
        newest = jnp.maximum(running, jnp.max(scores, axis=3))
        rescale = jnp.exp(running - newest)
        raised = jnp.exp(scores - newest[..., None])
        grad_probs = jnp.einsum(
            "qkgd,skd->kgqs", upstream_heads, values_now, preferred_element_type=jnp.float32
        )
        totals = totals * rescale + jnp.sum(raised, axis=3)
        delta_acc = delta_acc * rescale + jnp.sum(raised * grad_probs, axis=3)
        return ((newest, totals, delta_acc), None)

    start_stats = (
        jnp.full(stat_shape, -1e30, jnp.float32),
        jnp.zeros(stat_shape, jnp.float32),
        jnp.zeros(stat_shape, jnp.float32),
    )
    (running, totals, delta_acc), unused = lax.scan(stats_step, start_stats, block_ids)
    logsum = running + jnp.log(totals)
    deltas = delta_acc / totals

    def grad_pieces(block_index):
        keys_now, values_now, places_now = key_block(block_index)
        scores = block_scores(query_heads, keys_now, own_places, places_now, factor)
        weights = jnp.exp(scores - logsum[..., None])
        grad_probs = jnp.einsum(
            "qkgd,skd->kgqs", upstream_heads, values_now, preferred_element_type=jnp.float32
        )
        grad_scores = (weights * (grad_probs - deltas[..., None])).astype(jnp.bfloat16)
        return (keys_now, weights, grad_scores)

    query_zeros = jnp.zeros((own_rows, kv_heads, groups, HEAD_DIM), jnp.float32)

    def grad_step(carried, block_index):
        keys_now, weights, grad_scores = grad_pieces(block_index)
        carried = (
            carried
            + jnp.einsum(
                "kgqs,skd->qkgd", grad_scores, keys_now, preferred_element_type=jnp.float32
            )
            * factor
        )
        key_term = (
            jnp.einsum(
                "kgqs,qkgd->skd", grad_scores, query_heads, preferred_element_type=jnp.float32
            )
            * factor
        )
        value_term = jnp.einsum(
            "kgqs,qkgd->skd",
            weights.astype(jnp.bfloat16),
            upstream_heads,
            preferred_element_type=jnp.float32,
        )
        joined = jnp.concatenate(
            (key_term.reshape(block_rows, kv_width), value_term.reshape(block_rows, kv_width)),
            axis=1,
        )
        return (carried, joined)

    query_total, stacked = lax.scan(grad_step, query_zeros, block_ids)
    terms = stacked.reshape(seq_len, 2 * kv_width)
    mine = lax.psum_scatter(
        terms.astype(jnp.bfloat16), "cp", scatter_dimension=0, tiled=True
    ).astype(jnp.float32)
    key_grad = mine[:, :kv_width]
    value_grad = mine[:, kv_width:]
    query_grad = query_total.reshape(own_rows, kv_heads * groups * HEAD_DIM)
    return (query_grad, key_grad, value_grad)


MESH = pl.DeviceIdType.MESH
NT = (((1,), (1,)), ((), ()))
NN = (((1,), (0,)), ((), ()))
TILE = 256


def dot(a, b, dims):
    return lax.dot_general(a, b, dims, preferred_element_type=jnp.float32)


def neighbours(mine):
    partner = mine + 1 - 2 * lax.rem(mine, 2)
    return [mine, partner, lax.rem(mine + 2, 4), lax.rem(partner + 2, 4)]


def signal(peer):
    pl.semaphore_signal(
        pltpu.get_barrier_semaphore(), inc=1, device_id=peer, device_id_type=MESH
    )


def columns(ref, at, size):
    return ref.at[:, pl.ds(pl.multiple_of(at * size, size), size)]


def send_kernel(
    planes, kv_heads, cuts, pieces, q_ref, k_ref, v_ref, g_ref, w_ref, q_all, k_all, v_all, u_all,
    own_q, own_k, own_v, own_g, other_g, own_w, other_w, partial, u_buf,
    load_sem, own_sem, w_sem, g_sem, plane_sem, line_sem, kv_sem, q_sems, u_sems,
):
    me = lax.axis_index("cp")
    half = lax.axis_index("vocab")
    mine = lax.rem(me, kv_heads)
    plane = me // kv_heads
    first = plane * kv_heads
    end = planes - 1
    width = g_ref.shape[1]
    wide = width // kv_heads
    cut = wide // 2
    peers = neighbours(mine)
    order = [2, 3, 1, 0]
    steps = [(idx, part) for idx in order for part in range(2)]

    def w_copy(t, own):
        idx, part = steps[t]
        side = half if own else 1 - half
        return pltpu.make_async_copy(
            w_ref.at[
                pl.ds(pl.multiple_of(peers[idx] * wide + part * cut, cut), cut),
                pl.ds(pl.multiple_of(side * width, width), width),
            ],
            (own_w if own else other_w).at[t],
            w_sem.at[0 if own else 1, t],
        )

    loads = [
        pltpu.make_async_copy(source, target, load_sem.at[i])
        for i, (source, target) in enumerate(
            ((g_ref, own_g), (k_ref, own_k), (v_ref, own_v), (q_ref, own_q))
        )
    ]
    for copy in loads:
        copy.start()
    own_copies = [
        pltpu.make_async_copy(columns(q_ref, mine, wide), q_all.at[mine], own_sem.at[0]),
        pltpu.make_async_copy(columns(k_ref, mine, HEAD_DIM), k_all.at[me], own_sem.at[1]),
        pltpu.make_async_copy(columns(v_ref, mine, HEAD_DIM), v_all.at[me], own_sem.at[2]),
    ]
    for copy in own_copies:
        copy.start()
    signal({"vocab": 1 - half})
    for peer in peers[1:]:
        signal({"cp": first + peer})

    @pl.when(plane < end)
    def _():
        signal({"cp": me + kv_heads})

    @pl.when(plane > 0)
    def _():
        signal({"cp": me - kv_heads})

    lines = jnp.minimum(plane, 1) + jnp.minimum(end - plane, 1)
    for copy in loads:
        copy.wait()
    for own in (True, False):
        for t in range(len(steps)):
            w_copy(t, own).start()
    pl.semaphore_wait(pltpu.get_barrier_semaphore(), kv_heads + lines)

    def g_copy(n):
        r, inner, size = pieces[n]
        at = (pl.ds(*cuts[r]), pl.ds(inner, size))
        return pltpu.make_async_remote_copy(
            src_ref=own_g.at[at], dst_ref=other_g.at[at],
            send_sem=g_sem.at[0, n], recv_sem=g_sem.at[1, n],
            device_id={"vocab": 1 - half}, device_id_type=MESH,
        )

    def plane_copy(idx, i):
        return pltpu.make_async_remote_copy(
            src_ref=columns((own_k, own_v)[i], peers[idx], HEAD_DIM),
            dst_ref=(k_all, v_all)[i].at[me],
            send_sem=plane_sem.at[i, idx], recv_sem=kv_sem.at[i, me],
            device_id={"cp": first + peers[idx]}, device_id_type=MESH,
        )

    def line_copy(left, hops, idx, i):
        block = me - mine + peers[idx] + (kv_heads if left else -kv_heads) * hops
        kept = (k_all, v_all)[i]
        own = hops == 0 and idx == 0
        return pltpu.make_async_remote_copy(
            src_ref=columns((own_k, own_v)[i], mine, HEAD_DIM) if own else kept.at[block],
            dst_ref=kept.at[block],
            send_sem=line_sem.at[left, i, hops * kv_heads + idx], recv_sem=kv_sem.at[i, block],
            device_id={"cp": me + (-kv_heads if left else kv_heads)}, device_id_type=MESH,
        )

    def arrived(block):
        for i in range(2):
            slot = (k_all, v_all)[i].at[block]
            pltpu.make_async_remote_copy(
                src_ref=slot, dst_ref=slot,
                send_sem=plane_sem.at[i, 0], recv_sem=kv_sem.at[i, block],
                device_id={"cp": first + peers[1]}, device_id_type=MESH,
            ).wait_recv()

    def start_line(left, hops, idx):
        for i in range(2):
            line_copy(left, hops, idx, i).start()

    def open_line(idx):
        @pl.when(plane < end)
        def _():
            start_line(0, 0, idx)

        @pl.when(plane > 0)
        def _():
            start_line(1, 0, idx)

    def pass_plane(idx):
        arrived(first + peers[idx])
        open_line(idx)

    def pass_line(hops, idx):
        @pl.when((plane >= hops) & (plane < end))
        def _():
            arrived(first + peers[idx] - hops * kv_heads)
            start_line(0, hops, idx)

        @pl.when((plane <= end - hops) & (plane > 0))
        def _():
            arrived(first + peers[idx] + hops * kv_heads)
            start_line(1, hops, idx)

    def q_copy(idx):
        return pltpu.make_async_remote_copy(
            src_ref=columns(own_q, peers[idx], wide), dst_ref=q_all.at[mine],
            send_sem=q_sems.at[0, idx], recv_sem=q_sems.at[1, idx],
            device_id={"cp": first + peers[idx]}, device_id_type=MESH,
        )

    def u_copy(r, idx):
        rows = pl.ds(*cuts[r])
        return pltpu.make_async_remote_copy(
            src_ref=u_buf.at[idx, rows], dst_ref=u_all.at[mine, rows],
            send_sem=u_sems.at[0, r, idx], recv_sem=u_sems.at[1, r, idx],
            device_id={"cp": first + peers[idx]}, device_id_type=MESH,
        )

    for n in range(len(pieces)):
        g_copy(n).start()
    open_line(0)
    for idx in order[:-1]:
        for i in range(2):
            plane_copy(idx, i).start()
    for idx in order[:-1]:
        q_copy(idx).start()

    for t in range(len(steps)):
        w_copy(t, True).wait()
        partial[t] = dot(own_g[...], own_w[t], NT)
        if t in (0, 3, 6):
            pass_plane((0, 3, 6).index(t) + 1)
    events = [(hops, idx) for hops in range(1, end) for idx in range(kv_heads)]
    done = kv_heads - 1
    for hops, idx in events[:done]:
        pass_line(hops, idx)
    for n, (r, inner, size) in enumerate(pieces):
        rows = pl.ds(*cuts[r])
        depth = pl.ds(inner, size)
        g_copy(n).wait_recv()
        for t, (idx, part) in enumerate(steps):
            if n == 0:
                w_copy(t, False).wait()
            total = partial[t, rows] + dot(other_g[rows, depth], other_w[t, :, depth], NT)
            if inner + size < width:
                partial[t, rows] = total
            else:
                u_buf[idx, rows, pl.ds(part * cut, cut)] = total.astype(jnp.bfloat16)
                if part == 1 and idx != 0:
                    u_copy(r, idx).start()
            if (n, t) in ((0, 7), (1, 3), (1, 7), (2, 3), (2, 7)) and done < len(events):
                pass_line(*events[done])
                done += 1
    for hops, idx in events[done:]:
        pass_line(hops, idx)
    u_all[mine] = u_buf[0]

    for hops in range(1, planes):
        for idx in range(kv_heads):
            @pl.when(plane == end)
            def _():
                arrived(first + peers[idx] - hops * kv_heads)

            @pl.when(plane == 0)
            def _():
                arrived(first + peers[idx] + hops * kv_heads)

    for idx in order[:-1]:
        q_copy(idx).wait_recv()
        for r in range(len(cuts)):
            u_copy(r, idx).wait()
    for copy in own_copies:
        copy.wait()
    for n in range(len(pieces)):
        g_copy(n).wait_send()
    for idx in order[:-1]:
        q_copy(idx).wait_send()
        for i in range(2):
            plane_copy(idx, i).wait_send()
    for hops in range(end):
        for idx in range(kv_heads):
            for i in range(2):
                @pl.when((plane >= hops) & (plane < end))
                def _():
                    line_copy(0, hops, idx, i).wait_send()

                @pl.when((plane <= end - hops) & (plane > 0))
                def _():
                    line_copy(1, hops, idx, i).wait_send()


def score_kernel(
    order_ref, q_ref, k_ref, v_ref, u_ref, w_out, g_out, q_stack, u_stack,
    places, ks, vs, s_buf, p_buf,
):
    plane = lax.axis_index("cp") // q_ref.shape[0]
    own_rows = q_ref.shape[1]
    groups = q_ref.shape[2] // HEAD_DIM
    seq = k_ref.shape[0]
    spans = order_ref.shape[0]
    rows = seq // spans
    tile = groups * rows
    own_spans = q_ref.shape[0] * own_rows // rows
    per_block = own_rows // rows
    per_tile = TILE // rows
    scale = HEAD_DIM ** (-0.5) * 1.4426950408889634

    for r in range(spans):
        places[order_ref[r]] = r

    def place(j):
        return pl.ds(pl.multiple_of(places[j] * rows, rows), rows)

    for j in range(spans):
        for target, ref in ((ks, k_ref), (vs, v_ref)):
            target[pl.ds(j * rows, rows), :] = ref[place(j), :]

    def fold(x, op):
        return op(x.reshape(TILE // 8, 8, tile), axis=0)

    key_at = lax.broadcasted_iota(jnp.int32, (TILE, tile), 0)
    query_at = lax.rem(lax.broadcasted_iota(jnp.int32, (TILE, tile), 1), rows)

    def one_span(t, carry):
        block = t // per_block
        own = pl.ds(pl.multiple_of(lax.rem(t, per_block) * rows, rows), rows)
        cols = pl.ds(pl.multiple_of(t * tile, tile), tile)
        start = order_ref[plane * own_spans + t] * rows

        def stacked(ref):
            return jnp.concatenate(
                [ref[block, own, h * HEAD_DIM : (h + 1) * HEAD_DIM] for h in range(groups)], axis=0
            )

        def with_keys(last):
            q_tile = stacked(q_ref)
            u_tile = stacked(u_ref)
            q_stack[cols, :] = q_tile
            u_stack[cols, :] = u_tile
            peak = None
            for j in range(last + 1):
                keys = pl.ds(j * TILE, TILE)
                s = dot(ks[keys, :], q_tile, NT)
                if j == last:
                    s = jnp.where(key_at + (last * TILE - start) <= query_at, s, -1e30)
                s_buf[keys, :] = s
                top = fold(s, jnp.max)
                peak = top if peak is None else jnp.maximum(peak, top)
            peak = jnp.max(peak, axis=0, keepdims=True)
            total = jnp.zeros((8, tile), jnp.float32)
            delta = jnp.zeros((8, tile), jnp.float32)
            for j in range(last + 1):
                keys = pl.ds(j * TILE, TILE)
                p = jnp.exp2((s_buf[keys, :] - peak) * scale)
                dp = dot(vs[keys, :], u_tile, NT)
                total = total + fold(p, jnp.sum)
                delta = delta + fold(p * dp, jnp.sum)
                s_buf[keys, :] = p
                p_buf[keys, :] = dp
            inverse = 1.0 / jnp.sum(total, axis=0, keepdims=True)
            delta = jnp.sum(delta, axis=0, keepdims=True) * inverse
            for j in range(last + 1):
                keys = pl.ds(j * TILE, TILE)
                w = s_buf[keys, :] * inverse
                g = (w * (p_buf[keys, :] - delta)).astype(jnp.bfloat16)
                w = w.astype(jnp.bfloat16)
                for i in range(per_tile):
                    at = place(j * per_tile + i)
                    w_out[at, cols] = w[i * rows : (i + 1) * rows]
                    g_out[at, cols] = g[i * rows : (i + 1) * rows]
            blank = jnp.zeros((rows, tile), jnp.bfloat16)
            for j in range((last + 1) * per_tile, spans):
                w_out[place(j), cols] = blank
                g_out[place(j), cols] = blank

        for last in range(seq // TILE):
            pl.when(start // TILE == last)(functools.partial(with_keys, last))
        return carry

    lax.fori_loop(0, own_spans, one_span, 0)


def return_kernel(
    planes, kv_heads, w_ref, g_ref, q_ref, u_ref, k_ref, dq_all, dk_out, dv_out,
    k_turned, terms, summed, inbox, plane_box, dq_buf,
    send_sem, recv_sem, plane_sems, q_sems,
):
    me = lax.axis_index("cp")
    mine = lax.rem(me, kv_heads)
    plane = me // kv_heads
    first = plane * kv_heads
    end = planes - 1
    high = plane // 2
    outer = (plane == 0) | (plane == end)
    inner = 2 - high
    near = 1 + high
    peers = neighbours(mine)
    block_rows, wide = dq_buf.shape[1:]
    groups = wide // HEAD_DIM
    seq = g_ref.shape[0]
    tile = 2 * HEAD_DIM
    rows = tile // groups
    factor = HEAD_DIM ** (-0.5)

    for peer in peers[1:]:
        signal({"cp": first + peer})

    @pl.when(plane < end)
    def _():
        for m in range(kv_heads):
            signal({"cp": first + kv_heads + m})

    @pl.when(plane > 0)
    def _():
        for m in range(kv_heads):
            signal({"cp": first - kv_heads + m})

    def remote(source, target, sent, got, device):
        return pltpu.make_async_remote_copy(
            src_ref=source, dst_ref=target, send_sem=sent, recv_sem=got,
            device_id={"cp": device}, device_id_type=MESH,
        )

    def relay(source, stage, j, way, hops, device):
        slot = hops * kv_heads + j
        return remote(
            source, inbox.at[way, slot], send_sem.at[stage, j], recv_sem.at[way, slot],
            device * kv_heads + mine,
        )

    def final(source, stage, j, way, device):
        return remote(
            source, inbox.at[way, mine], send_sem.at[stage, j], recv_sem.at[way, mine],
            device * kv_heads + j,
        )

    def arrived(way, slot):
        at = inbox.at[way, slot]
        remote(at, at, send_sem.at[0, 0], recv_sem.at[way, slot], first + peers[1]).wait_recv()

    def chunk_of(i):
        return (1 - high) * (end - i) + high * i

    def compute(i):
        def one(j, carry):
            block = chunk_of(i) * kv_heads + j
            keys = pl.ds(pl.multiple_of(block * block_rows, block_rows), block_rows)
            dk = dot(g_ref[keys, :], q_ref[...], NN) * factor
            dv = dot(w_ref[keys, :], u_ref[...], NN)
            terms[block, :, :HEAD_DIM] = dk.astype(jnp.bfloat16)
            terms[block, :, HEAD_DIM:] = dv.astype(jnp.bfloat16)
            return carry

        lax.fori_loop(0, kv_heads, one, 0)

    def outward(i, j):
        source = terms.at[chunk_of(i) * kv_heads + j]
        if i == end - 1:
            return final(source, i, j, high, near)
        return relay(source, i, j, high, end - 1 - i, near)

    def plane_copy(idx):
        return remote(
            terms.at[first + peers[idx]], plane_box.at[mine],
            plane_sems.at[0, idx], plane_sems.at[1, mine], first + peers[idx],
        )

    def plane_arrived(idx):
        at = plane_box.at[peers[idx]]
        remote(at, at, plane_sems.at[0, idx], plane_sems.at[1, peers[idx]], first + peers[idx]).wait_recv()

    def dq_copy(idx):
        return remote(
            dq_buf.at[peers[idx]], columns(dq_all, mine, wide),
            q_sems.at[0, idx], q_sems.at[1, idx], first + peers[idx],
        )

    for i in range(planes):
        compute(i)
        if i == 0:
            lines = jnp.minimum(plane, 1) + jnp.minimum(end - plane, 1)
            pl.semaphore_wait(
                pltpu.get_barrier_semaphore(), kv_heads - 1 + kv_heads * lines
            )
        if i < end:
            @pl.when(outer)
            def _():
                for j in range(kv_heads):
                    outward(i, j).start()
    for idx in (2, 3, 1):
        plane_copy(idx).start()

    def middle(stage, way, slot, chunk, copy):
        for j in range(kv_heads):
            arrived(way, slot * kv_heads + j)
            total = terms[chunk * kv_heads + j].astype(jnp.float32) + inbox[
                way, slot * kv_heads + j
            ].astype(jnp.float32)
            summed[stage, j] = total.astype(jnp.bfloat16)
            copy(j).start()

    def onward(j):
        return relay(summed.at[0, j], 0, j, high, 1, inner)

    def to_end(j):
        return final(summed.at[1, j], 1, j, 1 - high, high * end)

    def to_inner(j):
        return final(summed.at[2, j], 2, j, high, inner)

    k_turned[...] = k_ref[...].T
    for t in range(seq // tile):
        cols = slice(t * tile, (t + 1) * tile)
        part = dot(k_turned[...], g_ref[:, cols], NN)
        part = (part.T * factor).astype(jnp.bfloat16)
        block, at = divmod(t * rows, block_rows)
        for h in range(groups):
            dq_buf[block, at : at + rows, h * HEAD_DIM : (h + 1) * HEAD_DIM] = part[
                h * rows : (h + 1) * rows
            ]
    for idx in (2, 3, 1):
        dq_copy(idx).start()

    @pl.when(jnp.logical_not(outer))
    def _():
        middle(0, high, 2, (1 - high) * end, onward)
        middle(1, 1 - high, 1, high * end, to_end)
        middle(2, high, 1, inner, to_inner)

    dq_all[:, pl.ds(pl.multiple_of(mine * wide, wide), wide)] = dq_buf[mine]
    plane_box[mine] = terms[me]

    def add(ref, m, value, fresh):
        cols = slice(m * HEAD_DIM, (m + 1) * HEAD_DIM)
        ref[:, cols] = value if fresh else ref[:, cols] + value

    def collect(box, m, fresh):
        value = box.astype(jnp.float32)
        add(dk_out, m, value[:, :HEAD_DIM], fresh)
        add(dv_out, m, value[:, HEAD_DIM:], fresh)

    for idx in range(1, kv_heads):
        plane_arrived(idx)
    for m in range(kv_heads):
        collect(plane_box[m], m, True)

    @pl.when(plane < end)
    def _():
        for m in range(kv_heads):
            arrived(1, m)
            collect(inbox[1, m], m, False)

    @pl.when(plane > 0)
    def _():
        for m in range(kv_heads):
            arrived(0, m)
            collect(inbox[0, m], m, False)

    for idx in range(1, kv_heads):
        plane_copy(idx).wait_send()
        dq_copy(idx).wait()

    @pl.when(outer)
    def _():
        for i in range(end):
            for j in range(kv_heads):
                outward(i, j).wait_send()

    @pl.when(jnp.logical_not(outer))
    def _():
        for copy in (onward, to_end, to_inner):
            for j in range(kv_heads):
                copy(j).wait_send()


def finish_kernel(dq_ref, dk_ref, dv_ref, dq_out, dk_out, dv_out, wide, sems):
    parts = wide.shape[0]
    rows = wide.shape[1]
    copies = [
        pltpu.make_async_copy(dk_ref, dk_out, sems.at[parts]),
        pltpu.make_async_copy(dv_ref, dv_out, sems.at[parts + 1]),
    ]
    for copy in copies:
        copy.start()
    for i in range(parts):
        at = pl.ds(i * rows, rows)
        wide[i] = dq_ref[at, :].astype(jnp.float32)
        copy = pltpu.make_async_copy(wide.at[i], dq_out.at[at], sems.at[i])
        copy.start()
        copies.append(copy)
    for copy in copies:
        copy.wait()


def by_planes(n, queries, key_states, value_states, out_grad, o_weight, span_order):
    own_rows, width = queries.shape
    kv_heads = key_states.shape[1] // HEAD_DIM
    planes = n // kv_heads
    wide = width // kv_heads
    cut = wide // 2
    seq = own_rows * n
    tile = (HEADS // KV_HEADS) * (seq // span_order.shape[0])
    stack = kv_heads * own_rows * (HEADS // KV_HEADS)
    quarter = own_rows // 4
    cuts = ((0, 2 * quarter), (2 * quarter, 2 * quarter))
    split = width // 2
    pieces = tuple((r, inner, split) for r in range(len(cuts)) for inner in (0, split))
    any_spec = pl.BlockSpec(memory_space=pl.ANY)
    vmem_spec = pl.BlockSpec(memory_space=pltpu.VMEM)
    smem_spec = pl.BlockSpec(memory_space=pltpu.SMEM)
    dma = pltpu.SemaphoreType.DMA
    low = jnp.bfloat16
    q_block = pltpu.VMEM((kv_heads, own_rows, wide), low)
    kv_block = pltpu.VMEM((n, own_rows, HEAD_DIM), low)
    q_all, k_all, v_all, u_all = pl.pallas_call(
        functools.partial(send_kernel, planes, kv_heads, cuts, pieces),
        out_shape=(q_block, kv_block, kv_block, q_block),
        in_specs=[any_spec] * 5,
        out_specs=(vmem_spec,) * 4,
        scratch_shapes=[
            pltpu.VMEM((own_rows, width), low),
            pltpu.VMEM(key_states.shape, low),
            pltpu.VMEM(key_states.shape, low),
            pltpu.VMEM((own_rows, width), low),
            pltpu.VMEM((own_rows, width), low),
            pltpu.VMEM((2 * kv_heads, cut, width), low),
            pltpu.VMEM((2 * kv_heads, cut, width), low),
            pltpu.VMEM((2 * kv_heads, own_rows, cut), jnp.float32),
            pltpu.VMEM((kv_heads, own_rows, wide), low),
            dma((4,)),
            dma((3,)),
            dma((2, 2 * kv_heads)),
            dma((2, len(pieces))),
            dma((2, kv_heads)),
            dma((2, 2, (planes - 1) * kv_heads)),
            dma((2, n)),
            dma((2, kv_heads)),
            dma((2, len(cuts), kv_heads)),
        ],
        compiler_params=pltpu.CompilerParams(
            collective_id=0, has_side_effects=True, vmem_limit_bytes=SEND_LIMIT
        ),
        name="send_heads",
    )(queries, key_states, value_states, out_grad, o_weight)
    k_all = k_all.reshape(seq, HEAD_DIM)
    pair = jax.ShapeDtypeStruct((seq, stack), low)
    side = jax.ShapeDtypeStruct((stack, HEAD_DIM), low)
    weights, grads, q_stack, u_stack = pl.pallas_call(
        score_kernel,
        out_shape=(pair, pair, side, side),
        in_specs=[smem_spec] + [vmem_spec] * 4,
        out_specs=(vmem_spec,) * 4,
        scratch_shapes=[pltpu.SMEM(span_order.shape, jnp.int32)]
        + [pltpu.VMEM((seq, HEAD_DIM), low)] * 2
        + [pltpu.VMEM((seq, tile), jnp.float32)] * 2,
        compiler_params=pltpu.CompilerParams(vmem_limit_bytes=16 << 20),
        name="scores",
    )(span_order, q_all, k_all, v_all.reshape(seq, HEAD_DIM), u_all)
    term = (own_rows, 2 * HEAD_DIM)
    grad = jax.ShapeDtypeStruct(key_states.shape, jnp.float32)
    dq_all, key_grad, value_grad = pl.pallas_call(
        functools.partial(return_kernel, planes, kv_heads),
        out_shape=(jax.ShapeDtypeStruct((own_rows, width), low), grad, grad),
        in_specs=[vmem_spec] * 5,
        out_specs=(vmem_spec,) * 3,
        scratch_shapes=[
            pltpu.VMEM((HEAD_DIM, seq), low),
            pltpu.VMEM((n,) + term, low),
            pltpu.VMEM((3, kv_heads) + term, low),
            pltpu.VMEM((2, 3 * kv_heads) + term, low),
            pltpu.VMEM((kv_heads,) + term, low),
            pltpu.VMEM((kv_heads, own_rows, wide), low),
            dma((3, kv_heads)),
            dma((2, 3 * kv_heads)),
            dma((2, kv_heads)),
            dma((2, kv_heads)),
        ],
        compiler_params=pltpu.CompilerParams(
            collective_id=1, has_side_effects=True, vmem_limit_bytes=16 << 20
        ),
        name="return_grads",
    )(weights, grads, q_stack, u_stack, k_all)
    parts = 8
    return pl.pallas_call(
        finish_kernel,
        out_shape=(jax.ShapeDtypeStruct(queries.shape, jnp.float32), grad, grad),
        in_specs=[vmem_spec] * 3,
        out_specs=(any_spec,) * 3,
        scratch_shapes=[
            pltpu.VMEM((parts, own_rows // parts, width), jnp.float32),
            dma((parts + 2,)),
        ],
        compiler_params=pltpu.CompilerParams(vmem_limit_bytes=8 << 20),
        name="finish",
    )(dq_all, key_grad, value_grad)


SEND_LIMIT = 60 << 20


def solution(mesh):
    n = mesh.shape["cp"]
    planes = mesh.shape["vocab"] == 2 and n == 4 * (KV_HEADS // 2)
    body = functools.partial(by_planes, n) if planes else local
    return jax.shard_map(
        body,
        mesh=mesh,
        in_specs=(
            P("cp", "vocab"),
            P("cp", "vocab"),
            P("cp", "vocab"),
            P("cp", "vocab"),
            P("vocab", None),
            P(),
        ),
        out_specs=(P("cp", "vocab"), P("cp", "vocab"), P("cp", "vocab")),
        check_vma=False,
    )
```
